32 devices in a mesh: dp: 4 (over z), cp: 8 (over y, x, core).
Axes of the slice: x: 2, y: 2, z: 4, core: 2. Of those that a mesh axis runs over, the one named last changes fastest.
Arguments:
- x: bfloat16 [4096, 6144], P(('dp', 'cp')), parts along dimension 0
- k_cache: bfloat16 [65536, 8, 128], P(('dp', 'cp')), parts along dimension 0
- v_cache: bfloat16 [65536, 8, 128], P(('dp', 'cp')), parts along dimension 0
- ln_gain: bfloat16 [6144], replicated
- w_q: bfloat16 [6144, 12288], replicated
- w_k: bfloat16 [6144, 1024], replicated
- w_v: bfloat16 [6144, 1024], replicated
- w_o: bfloat16 [12288, 6144], replicated
- q_gain: bfloat16 [128], replicated
- k_gain: bfloat16 [128], replicated
Outputs:
- output 1: bfloat16 [4096, 6144], P(('dp', 'cp')), parts along dimension 0
- output 2: bfloat16 [4096, 8, 128], P(('dp', 'cp')), parts along dimension 0
- output 3: bfloat16 [4096, 8, 128], P(('dp', 'cp')), parts along dimension 0
There are 4 independent parts. The reference program is written for one: setup_inputs(seed, part) draws one part's arguments, and reference() takes and returns one part's arrays. A program takes and returns all parts, laid end to end along the dimension named above; an argument that names none is the same for every part.
All inputs are finite; a program needn't handle non-finite values.
Results may differ from the reference program's by a relative error of at most 0.0105903.
Values are sent between devices in bfloat16 or wider.
A program may use at most 1.5 GiB of HBM per device.

```python
import jax
import jax.numpy as jnp
from jax import lax

HIDDEN = 6144
Q_HEADS = 96
KV_HEADS = 8
HEAD_DIM = 128
NEW_LEN = 1024
PREFIX_LEN = 16384
ROW_BLOCK = 16
ROPE_THETA = 1.0e6
NORM_EPS = 1.0e-6


def setup_inputs(seed: int = 0, part: int = 0) -> dict:
    part_key = jax.random.fold_in(jax.random.key(seed), part)
    part_keys = jax.random.split(part_key, 3)
    shared = jax.random.split(jax.random.key(seed + 1), 7)
    q_width = Q_HEADS * HEAD_DIM
    kv_width = KV_HEADS * HEAD_DIM
    total_len = PREFIX_LEN + NEW_LEN
    x = jax.random.normal(part_keys[0], (NEW_LEN, HIDDEN), jnp.float32)
    k_cache = jax.random.normal(part_keys[1], (PREFIX_LEN, KV_HEADS, HEAD_DIM), jnp.float32)
    v_cache = jax.random.normal(part_keys[2], (PREFIX_LEN, KV_HEADS, HEAD_DIM), jnp.float32)
    ln_gain = 1.0 + 0.4 * jax.random.normal(shared[0], (HIDDEN,), jnp.float32)
    w_q = jax.random.normal(shared[1], (HIDDEN, q_width), jnp.float32) * HIDDEN ** -0.5
    w_k = jax.random.normal(shared[2], (HIDDEN, kv_width), jnp.float32) * HIDDEN ** -0.5
    w_v = jax.random.normal(shared[3], (HIDDEN, kv_width), jnp.float32) * HIDDEN ** -0.5
    w_o = jax.random.normal(shared[4], (q_width, HIDDEN), jnp.float32) * (0.5 * (total_len / q_width) ** 0.5)
    q_gain = 1.0 + 0.3 * jax.random.normal(shared[5], (HEAD_DIM,), jnp.float32)
    k_gain = 1.5 + 0.3 * jax.random.normal(shared[6], (HEAD_DIM,), jnp.float32)
    return {'x': x.astype(jnp.bfloat16), 'k_cache': k_cache.astype(jnp.bfloat16), 'v_cache': v_cache.astype(jnp.bfloat16), 'ln_gain': ln_gain.astype(jnp.bfloat16), 'w_q': w_q.astype(jnp.bfloat16), 'w_k': w_k.astype(jnp.bfloat16), 'w_v': w_v.astype(jnp.bfloat16), 'w_o': w_o.astype(jnp.bfloat16), 'q_gain': q_gain.astype(jnp.bfloat16), 'k_gain': k_gain.astype(jnp.bfloat16)}


def rms_norm(vals, gain):
    mean_sq = jnp.mean(vals * vals, axis=-1, keepdims=True)
    return vals * lax.rsqrt(mean_sq + NORM_EPS) * gain


def apply_rope(vals, positions):
    half = HEAD_DIM // 2
    inv_freq = ROPE_THETA ** (-jnp.arange(half, dtype=jnp.float32) * (2.0 / HEAD_DIM))
    angles = positions.astype(jnp.float32)[:, None] * inv_freq[None, :]
    cos_tab = jnp.cos(angles)[:, None, :]
    sin_tab = jnp.sin(angles)[:, None, :]
    first = vals[..., :half]
    second = vals[..., half:]
    return jnp.concatenate([first * cos_tab - second * sin_tab, second * cos_tab + first * sin_tab], axis=-1)


def reference(x, k_cache, v_cache, ln_gain, w_q, w_k, w_v, w_o, q_gain, k_gain):
    group = Q_HEADS // KV_HEADS
    scale = HEAD_DIM ** -0.5
    x_wide = x.astype(jnp.float32)
    hidden = rms_norm(x_wide, ln_gain.astype(jnp.float32)).astype(jnp.bfloat16)
    q_raw = jnp.dot(hidden, w_q, preferred_element_type=jnp.float32).astype(jnp.bfloat16)
    k_raw = jnp.dot(hidden, w_k, preferred_element_type=jnp.float32).astype(jnp.bfloat16)
    v_new = jnp.dot(hidden, w_v, preferred_element_type=jnp.float32).astype(jnp.bfloat16).reshape(NEW_LEN, KV_HEADS, HEAD_DIM)
    positions = PREFIX_LEN + jnp.arange(NEW_LEN)
    q_rot = apply_rope(rms_norm(q_raw.reshape(NEW_LEN, Q_HEADS, HEAD_DIM).astype(jnp.float32), q_gain.astype(jnp.float32)), positions).astype(jnp.bfloat16)
    k_new = apply_rope(rms_norm(k_raw.reshape(NEW_LEN, KV_HEADS, HEAD_DIM).astype(jnp.float32), k_gain.astype(jnp.float32)), positions).astype(jnp.bfloat16)
    keys_all = jnp.concatenate([k_cache, k_new], axis=0).astype(jnp.float32)
    values_all = jnp.concatenate([v_cache, v_new], axis=0).astype(jnp.float32)
    key_pos = jnp.arange(PREFIX_LEN + NEW_LEN)
    block_count = NEW_LEN // ROW_BLOCK
    q_blocks = q_rot.reshape(block_count, ROW_BLOCK, KV_HEADS, group, HEAD_DIM)

    def block_attend(block):
        q_block, block_index = block
        row_pos = PREFIX_LEN + block_index * ROW_BLOCK + jnp.arange(ROW_BLOCK)
        scores = jnp.einsum('rkgd,skd->rkgs', q_block.astype(jnp.float32), keys_all) * scale
        allowed = key_pos[None, :] <= row_pos[:, None]
        scores = jnp.where(allowed[:, None, None, :], scores, -jnp.inf)
        peak = jnp.max(scores, axis=-1, keepdims=True)
        weights = jnp.exp(scores - peak)
        probs = weights / jnp.sum(weights, axis=-1, keepdims=True)
        return jnp.einsum('rkgs,skd->rkgd', probs, values_all)

    attended = lax.map(block_attend, (q_blocks, jnp.arange(block_count)))
    attended = attended.reshape(NEW_LEN, Q_HEADS * HEAD_DIM).astype(jnp.bfloat16)
    out = (x_wide + jnp.dot(attended, w_o, preferred_element_type=jnp.float32)).astype(jnp.bfloat16)
    return (out, k_new, v_new)
```

```python
import functools
import math

import jax
import jax.numpy as jnp
from jax import lax
from jax.experimental import pallas as pl
from jax.experimental.pallas import tpu as pltpu
from jax.sharding import PartitionSpec as P

HEAD_DIM = 128
ROPE_THETA = 1.0e6
NORM_EPS = 1.0e-6
MESH = pl.DeviceIdType.MESH
F32 = jnp.float32
BF16 = jnp.bfloat16

ORD = (0, 1, 2, 4, 3, 5, 6, 7)
SUB = 256
HEADS_PER_TILE = 4


def rms_norm(vals, gain):
    mean_sq = jnp.mean(vals * vals, axis=-1, keepdims=True)
    return vals * lax.rsqrt(mean_sq + NORM_EPS) * gain


def apply_rope(vals, positions):
    half = HEAD_DIM // 2
    inv_freq = ROPE_THETA ** (-jnp.arange(half, dtype=F32) * (2.0 / HEAD_DIM))
    angles = positions.astype(F32)[:, None] * inv_freq[None, :]
    cos_tab = jnp.cos(angles)[:, None, :]
    sin_tab = jnp.sin(angles)[:, None, :]
    first = vals[..., :half]
    second = vals[..., half:]
    return jnp.concatenate([first * cos_tab - second * sin_tab, second * cos_tab + first * sin_tab], axis=-1)


def project_rows(x_wide, ln_gain, w_q, w_k, w_v, q_gain, k_gain, positions):
    rows = x_wide.shape[0]
    hidden = rms_norm(x_wide, ln_gain.astype(F32)).astype(BF16)
    q_raw = jnp.dot(hidden, w_q, preferred_element_type=F32).astype(BF16).reshape(rows, -1, HEAD_DIM)
    k_raw = jnp.dot(hidden, w_k, preferred_element_type=F32).astype(BF16).reshape(rows, -1, HEAD_DIM)
    v_new = jnp.dot(hidden, w_v, preferred_element_type=F32).astype(BF16).reshape(rows, -1, HEAD_DIM)
    q_rot = apply_rope(rms_norm(q_raw.astype(F32), q_gain.astype(F32)), positions).astype(BF16)
    k_new = apply_rope(rms_norm(k_raw.astype(F32), k_gain.astype(F32)), positions).astype(BF16)
    return q_rot, k_new, v_new


def flip(me, rel):
    out = 0
    for bit in (1, 2, 4):
        mine = (me // bit) % 2
        out = out + bit * ((1 - mine) if rel & bit else mine)
    return out


def attn_kernel(rows, seg, width, q_in, kt, vt, kn, vn, o_out,
                qbuf, kbuf, vbuf, ostage, scores, acc, peak_ref, sum_ref, chunk_max, send, recv):
    dp = lax.axis_index("dp")
    me = lax.axis_index("cp")
    new = 8 * rows
    cols = HEADS_PER_TILE * rows
    tiles_per_slot = width // (HEADS_PER_TILE * HEAD_DIM)
    tiles = 8 * tiles_per_slot
    keys_a = 2 * seg
    keys_b = 2 * seg + new
    coef = math.log2(math.e) * HEAD_DIM ** -0.5
    neg = float("-inf")

    barrier = pltpu.get_barrier_semaphore()
    for rel in range(1, 8):
        pl.semaphore_signal(barrier, inc=1, device_id=(dp, flip(me, rel)), device_id_type=MESH)
    pl.semaphore_wait(barrier, 7)

    def qcols(who):
        return pl.ds(pl.multiple_of(who * width, width), width)

    def pieces(p):
        peer = flip(me, ORD[p])
        return {
            "q": (0, q_in.at[:, qcols(peer)], qbuf.at[p]),
            "k": (1, kt.at[peer], kbuf.at[pl.ds(p * seg, seg), :]),
            "v": (2, vt.at[peer], vbuf.at[:, pl.ds(p * seg, seg)]),
            "kn": (3, kn.at[peer], kbuf.at[pl.ds(pl.multiple_of(8 * seg + me * rows, rows), rows), :]),
            "vn": (4, vn.at[peer], vbuf.at[:, pl.ds(pl.multiple_of(8 * seg + me * rows, rows), rows)]),
            "o": (5, ostage.at[p], o_out.at[:, qcols(me)]),
        }

    def copy_of(p, what):
        kind, src, dst = pieces(p)[what]
        if p == 0:
            return pltpu.make_async_copy(src, dst, recv.at[kind, 0])
        return pltpu.make_async_remote_copy(
            src_ref=src, dst_ref=dst, send_sem=send.at[kind, p], recv_sem=recv.at[kind, p],
            device_id=(dp, flip(me, ORD[p])), device_id_type=MESH)

    def wait_in(p, what):
        c = copy_of(p, what)
        if p == 0:
            c.wait()
        else:
            c.wait_recv()

    for p in range(8):
        copy_of(p, "q").start()
        if p < 2:
            copy_of(p, "k").start()
            copy_of(p, "v").start()
    for p in range(2, 8):
        copy_of(p, "k").start()
        copy_of(p, "v").start()
    for p in range(8):
        copy_of(p, "kn").start()
        copy_of(p, "vn").start()

    def init(t, carry):
        peak_ref[t] = jnp.full((1, cols), neg, F32)
        sum_ref[t] = jnp.zeros((1, cols), F32)
        acc[t] = jnp.zeros((HEAD_DIM, cols), F32)
        return carry

    lax.fori_loop(0, tiles, init, 0)

    def q_tile(t):
        slot, part = t // tiles_per_slot, t % tiles_per_slot
        first = pl.multiple_of(part * HEADS_PER_TILE * HEAD_DIM, HEADS_PER_TILE * HEAD_DIM)
        block = qbuf[slot, :, pl.ds(first, HEADS_PER_TILE * HEAD_DIM)]
        return jnp.concatenate(
            [block[:, h * HEAD_DIM:(h + 1) * HEAD_DIM] for h in range(HEADS_PER_TILE)], axis=0)

    def step(pv=None, qk=None):
        if pv is not None:
            t, base, keys_p = pv
            old = peak_ref[t]
            top = jnp.maximum(old, jnp.max(chunk_max[...], axis=0, keepdims=True) * coef)
            fade = jnp.exp2(old - top)
            peak_ref[t] = top
        if qk is not None:
            tq, base_q, keys_q, owner = qk
            q = q_tile(tq)
        total = None
        values = None
        peaks = None
        for s in range(max(pv[2] if pv else 0, qk[2] if qk else 0) // SUB):
            lines = slice(s * SUB, (s + 1) * SUB)
            if pv is not None and s * SUB < keys_p:
                w = jnp.exp2(scores[lines, :] * coef - top)
                part = jnp.sum(w.reshape(SUB // 8, 8, cols), axis=0)
                total = part if total is None else total + part
                v_part = vbuf[:, pl.ds(pl.multiple_of(base + s * SUB, SUB), SUB)]
                o_part = jnp.dot(v_part, w.astype(BF16), preferred_element_type=F32)
                values = o_part if values is None else values + o_part
            if qk is not None and s * SUB < keys_q:
                k_part = kbuf[pl.ds(pl.multiple_of(base_q + s * SUB, SUB), SUB), :]
                sc = lax.dot_general(k_part, q, (((1,), (1,)), ((), ())), preferred_element_type=F32)
                if owner is not None and s * SUB >= keys_a:
                    key = lax.broadcasted_iota(jnp.int32, (SUB, cols), 0) + (s * SUB - keys_a)
                    row = lax.broadcasted_iota(jnp.int32, (SUB, cols), 1) % rows + owner * rows
                    sc = jnp.where(key <= row, sc, neg)
                scores[lines, :] = sc
                part = jnp.max(sc.reshape(SUB // 8, 8, cols), axis=0)
                peaks = part if peaks is None else jnp.maximum(peaks, part)
        if qk is not None:
            chunk_max[...] = peaks
        if pv is None:
            return None
        sums = sum_ref[t] * fade + jnp.sum(total, axis=0, keepdims=True)
        return sums, acc[t] * fade + values

    def keep(t, result):
        sum_ref[t], acc[t] = result

    def finish(t, result):
        sums, whole = result
        done = whole / sums
        slot, part = t // tiles_per_slot, t % tiles_per_slot
        first = pl.multiple_of(part * HEADS_PER_TILE * HEAD_DIM, HEADS_PER_TILE * HEAD_DIM)
        ostage[slot, :, pl.ds(first, HEADS_PER_TILE * HEAD_DIM)] = jnp.concatenate(
            [done[:, h * rows:(h + 1) * rows].T.astype(BF16) for h in range(HEADS_PER_TILE)], axis=1)

    for p in (0, 1):
        wait_in(p, "q") if p == 0 else None
        wait_in(p, "k")
        wait_in(p, "v")
    step(qk=(0, 0, keys_a, None))
    steps_a = 3 * tiles

    def body_a(i, carry):
        for p in range(1, 8):
            @pl.when(i + 1 == p * tiles_per_slot)
            def _():
                wait_in(p, "q")
        for v in (1, 2):
            @pl.when(i + 1 == v * tiles)
            def _():
                for p in (2 * v, 2 * v + 1):
                    wait_in(p, "k")
                    wait_in(p, "v")
        nxt = i + 1
        t = i % tiles
        keep(t, step(pv=(t, (i // tiles) * keys_a, keys_a),
                     qk=(nxt % tiles, (nxt // tiles) * keys_a, keys_a, None)))
        return carry

    lax.fori_loop(0, steps_a - 1, body_a, 0)

    for p in (6, 7):
        wait_in(p, "k")
        wait_in(p, "v")
    for p in range(8):
        wait_in(p, "kn")
        wait_in(p, "vn")

    def tile_b(i):
        return (7 - i // tiles_per_slot) * tiles_per_slot + i % tiles_per_slot

    def owner_of(i):
        slot = 7 - i // tiles_per_slot
        b0, b1, b2 = slot % 2, (slot // 2) % 2, slot // 4
        swap = b0 * b1 * (1 - b2) + (1 - b0) * (1 - b1) * b2
        r0 = (b0 + swap) % 2
        r1 = (b1 + swap) % 2
        r2 = (b2 + swap) % 2
        return (me % 2 + r0) % 2 + 2 * ((me // 2 + r1) % 2) + 4 * ((me // 4 + r2) % 2)

    last_t = tiles - 1
    base_b = 3 * keys_a
    keep(last_t, step(pv=(last_t, 2 * keys_a, keys_a), qk=(tile_b(0), base_b, keys_b, owner_of(0))))

    def body_b(i, carry):
        for p in range(7, 0, -1):
            @pl.when(i == (8 - p) * tiles_per_slot)
            def _():
                copy_of(p, "o").start()
        t = tile_b(i)
        finish(t, step(pv=(t, base_b, keys_b), qk=(tile_b(i + 1), base_b, keys_b, owner_of(i + 1))))
        return carry

    lax.fori_loop(0, tiles - 1, body_b, 0)
    t = tiles_per_slot - 1
    finish(t, step(pv=(t, base_b, keys_b)))
    copy_of(0, "o").start()
    for p in range(8):
        wait_in(p, "o")
    for p in range(1, 8):
        for what in ("q", "k", "v", "kn", "vn", "o"):
            copy_of(p, what).wait_send()


def attend(q, kt, vt, kn, vn):
    rows = q.shape[0]
    kv_heads, seg, _ = kt.shape
    width = q.shape[1] // kv_heads
    new = 8 * rows
    cols = HEADS_PER_TILE * rows
    tiles = 8 * width // (HEADS_PER_TILE * HEAD_DIM)
    keys_b = 2 * seg + new
    flops = 4 * (8 * seg + new) * 8 * rows * width
    return pl.pallas_call(
        functools.partial(attn_kernel, rows, seg, width),
        out_shape=jax.ShapeDtypeStruct(q.shape, BF16),
        in_specs=[pl.BlockSpec(memory_space=pl.ANY)] * 5,
        out_specs=pl.BlockSpec(memory_space=pl.ANY),
        scratch_shapes=[
            pltpu.VMEM((8, rows, width), BF16),
            pltpu.VMEM((8 * seg + new, HEAD_DIM), BF16),
            pltpu.VMEM((HEAD_DIM, 8 * seg + new), BF16),
            pltpu.VMEM((8, rows, width), BF16),
            pltpu.VMEM((keys_b, cols), F32),
            pltpu.VMEM((tiles, HEAD_DIM, cols), F32),
            pltpu.VMEM((tiles, 1, cols), F32),
            pltpu.VMEM((tiles, 1, cols), F32),
            pltpu.VMEM((8, cols), F32),
            pltpu.SemaphoreType.DMA((6, 8)),
            pltpu.SemaphoreType.DMA((6, 8)),
        ],
        compiler_params=pltpu.CompilerParams(
            collective_id=0, has_side_effects=True, vmem_limit_bytes=60 * 1024 * 1024),
        cost_estimate=pl.CostEstimate(flops=flops, bytes_accessed=32 * 1024 * 1024, transcendentals=flops // 512),
        name="attend",
    )(q, kt, vt, kn, vn)


def solution(mesh):
    cp_size = mesh.shape['cp']
    row_spec = P(('dp', 'cp'), None)
    cache_spec = P(('dp', 'cp'), None, None)
    whole = P()

    def device_step(x_rows, k_cache, v_cache, ln_gain, w_q, w_k, w_v, w_o, q_gain, k_gain):
        rows = x_rows.shape[0]
        prefix_len = k_cache.shape[0] * cp_size
        my_index = lax.axis_index('cp')
        row_ids = my_index * rows + jnp.arange(rows)
        x_wide = x_rows.astype(F32)
        q_rot, k_new, v_new = project_rows(x_wide, ln_gain, w_q, w_k, w_v, q_gain, k_gain, prefix_len + row_ids)
        attended = attend(
            q_rot.reshape(rows, -1),
            jnp.transpose(k_cache, (1, 0, 2)),
            jnp.transpose(v_cache, (1, 2, 0)),
            jnp.transpose(k_new, (1, 0, 2)),
            jnp.transpose(v_new, (1, 2, 0)),
        )
        out = (x_wide + jnp.dot(attended, w_o, preferred_element_type=F32)).astype(BF16)
        return out, k_new, v_new

    return jax.shard_map(device_step, mesh=mesh, in_specs=(row_spec, cache_spec, cache_spec, whole, whole, whole, whole, whole, whole, whole), out_specs=(row_spec, cache_spec, cache_spec), check_vma=False)
```

```python
import functools
import math

import jax
import jax.numpy as jnp
from jax import lax
from jax.experimental import pallas as pl
from jax.experimental.pallas import tpu as pltpu
from jax.sharding import PartitionSpec as P

HEAD_DIM = 128
ROPE_THETA = 1.0e6
NORM_EPS = 1.0e-6
MESH = pl.DeviceIdType.MESH
F32 = jnp.float32
BF16 = jnp.bfloat16

ORD = (0, 1, 2, 4, 3, 5, 6, 7)
SUB = 256
TILE = 512
HEADS = TILE // HEAD_DIM
WBUFS = 3


def flip(me, rel):
    out = 0
    for bit in (1, 2, 4):
        mine = (me // bit) % 2
        out = out + bit * ((1 - mine) if rel & bit else mine)
    return out


def flip_chip(chip, rel):
    return (chip % 2 + rel % 2) % 2 + 2 * ((chip // 2 + rel // 2) % 2)


def block_kernel(rows, seg, width,
                 x_in, kt, vt, ln_in, gain_in, cos_in, sin_in, wq_in, wk_in, wv_in, wo_in,
                 out, k_out, v_out,
                 xbuf, hbuf, wbuf, raw, stage, vstage, qbuf, kbuf, vbuf, scores, acc, peak_ref, sum_ref, chunk_max, outst,
                 wsem, xsem, qsend, qrecv, kvsend, kvrecv, nsend, nrecv, osend, orecv, ksend, krecv, psend, precv, outsem,
                 free_sem):
    dp = lax.axis_index("dp")
    me = lax.axis_index("cp")
    chip, core = me // 2, me % 2
    hid = wbuf.shape[1]
    pair = 2 * rows
    new = 8 * rows
    parts = width // TILE
    per_chip = 2 * parts
    tiles = 4 * per_chip
    keys_a = 2 * seg
    keys_b = 2 * seg + new
    coef = math.log2(math.e) * HEAD_DIM ** -0.5
    neg = float("-inf")
    q_tiles = 4 * parts
    p1_tiles = q_tiles + 2
    out_tiles = hid // TILE
    chunk = hid // 4

    def device(index):
        return (dp, index)

    partner = flip(me, 1)

    barrier = pltpu.get_barrier_semaphore()
    for rel in range(1, 8):
        pl.semaphore_signal(barrier, inc=1, device_id=device(flip(me, rel)), device_id_type=MESH)
    pl.semaphore_wait(barrier, 7)

    def remote(src, dst, send, recv, index):
        return pltpu.make_async_remote_copy(
            src_ref=src, dst_ref=dst, send_sem=send, recv_sem=recv, device_id=device(index), device_id_type=MESH)

    my_rows = pl.ds(pl.multiple_of(core * rows, rows), rows)
    other_rows = pl.ds(pl.multiple_of((1 - core) * rows, rows), rows)

    def tile_of(ref, slot, a):
        return ref.at[slot, pl.ds(a * chunk, chunk), :]

    def fetch_kv(ref, n):
        slot = n % WBUFS
        for a in range(4):
            first = pl.multiple_of((2 * a + core) * HEAD_DIM, HEAD_DIM)
            pltpu.make_async_copy(ref.at[:, pl.ds(first, HEAD_DIM)],
                                  wbuf.at[slot, :, pl.ds(a * HEAD_DIM, HEAD_DIM)], wsem.at[slot, a]).start()

    def fetch_q(n):
        slot = n % WBUFS
        g, part = (n - 1) // parts, (n - 1) % parts
        head = 2 * flip_chip(chip, (g + 1) % 4) + core
        first = pl.multiple_of(head * width + part * TILE, TILE)
        for a in range(4):
            pltpu.make_async_copy(wq_in.at[pl.ds(a * chunk, chunk), pl.ds(first, TILE)],
                                  tile_of(wbuf, slot, a), wsem.at[slot, a]).start()

    def fetch_o(m):
        slot = (p1_tiles + m) % WBUFS
        first = pl.multiple_of(m * TILE, TILE)
        for a in range(4):
            top = pl.multiple_of((2 * a + core) * width, width)
            pltpu.make_async_copy(wo_in.at[pl.ds(top, width), pl.ds(first, TILE)],
                                  tile_of(wbuf, slot, a), wsem.at[slot, a]).start()

    def wait_tile(n):
        slot = n % WBUFS
        for a in range(4):
            pltpu.make_async_copy(tile_of(wbuf, slot, a), tile_of(wbuf, slot, a), wsem.at[slot, a]).wait()

    x_local = pltpu.make_async_copy(x_in, xbuf.at[my_rows, :], xsem.at[0])
    x_remote = remote(x_in, xbuf.at[my_rows, :], xsem.at[1], xsem.at[2], partner)
    x_local.start()
    x_remote.start()
    fetch_kv(wk_in, 0)
    fetch_q(1)
    fetch_q(2)

    def kv_copy(p, kind):
        peer = flip(me, ORD[p])
        if kind == 0:
            src, dst = kt.at[peer], kbuf.at[pl.ds(p * seg, seg), :]
        else:
            src, dst = vt.at[peer], vbuf.at[:, pl.ds(p * seg, seg)]
        if p == 0:
            return pltpu.make_async_copy(src, dst, kvrecv.at[kind, 0])
        return remote(src, dst, kvsend.at[kind, p], kvrecv.at[kind, p], peer)

    def kv_wait(p):
        for kind in range(2):
            if p == 0:
                kv_copy(p, kind).wait()
            else:
                kv_copy(p, kind).wait_recv()

    for p in range(2):
        for kind in range(2):
            kv_copy(p, kind).start()

    def normalise(first_row):
        def some(i, carry):
            at = pl.multiple_of(first_row + i * 16, 16)
            wide = xbuf[pl.ds(at, 16), :].astype(F32)
            mean_sq = jnp.sum(wide * wide, axis=-1, keepdims=True) * (1.0 / hid)
            hbuf[pl.ds(at, 16), :] = (wide * lax.rsqrt(mean_sq + NORM_EPS) * ln_in[...]).astype(BF16)
            return carry
        lax.fori_loop(0, rows // 16, some, 0)

    x_local.wait()
    normalise(core * rows)
    x_remote.wait_recv()
    normalise((1 - core) * rows)

    def multiply(n):
        slot = n % WBUFS
        return jnp.dot(hbuf[...], wbuf[slot], preferred_element_type=F32)

    def rotate(e):
        group, part = (e + parts - 1) // parts, (e + parts - 1) % parts
        gain = gain_in[jnp.minimum(e, 1)]
        cos_tab, sin_tab = cos_in[...], sin_in[...]
        done = []
        for h in range(HEADS):
            vals = raw[:, h * HEAD_DIM:(h + 1) * HEAD_DIM].astype(F32)
            mean_sq = jnp.sum(vals * vals, axis=-1, keepdims=True) * (1.0 / HEAD_DIM)
            vals = vals * lax.rsqrt(mean_sq + NORM_EPS) * gain
            done.append((vals * cos_tab + pltpu.roll(vals, HEAD_DIM // 2, 1) * sin_tab).astype(BF16))
        done = jnp.concatenate(done, axis=1)
        where = pl.ds(pl.multiple_of(part * TILE, TILE), TILE)
        stage[group, :, where] = done
        qbuf[0, :, where] = done

    def q_copy(rel, part):
        cols = pl.ds(pl.multiple_of(part * TILE, TILE), TILE)
        return remote(stage.at[rel, :, cols], qbuf.at[rel, :, cols], qsend.at[rel, part], qrecv.at[rel, part],
                      2 * flip_chip(chip, rel) + core)

    def new_copy(rel, kind):
        other = flip_chip(chip, rel)
        here = pl.ds(pl.multiple_of(8 * seg + chip * pair, pair), pair)
        if kind == 0:
            first = pl.multiple_of((parts - 1) * TILE + other * HEAD_DIM, HEAD_DIM)
            src, dst = stage.at[0, :, pl.ds(first, HEAD_DIM)], kbuf.at[here, :]
        else:
            src, dst = vstage.at[other], vbuf.at[:, here]
        return remote(src, dst, nsend.at[kind, rel], nrecv.at[kind, rel], 2 * other + core)

    k_cols = pl.ds((parts - 1) * TILE, TILE)
    new_outs = (
        (pltpu.make_async_copy(stage.at[0, my_rows, k_cols], k_out.at[core], krecv.at[0]),
         remote(stage.at[0, other_rows, k_cols], k_out.at[core], ksend.at[0], krecv.at[1], partner)),
        (pltpu.make_async_copy(raw.at[my_rows, :], v_out.at[core], krecv.at[2]),
         remote(raw.at[other_rows, :], v_out.at[core], ksend.at[1], krecv.at[3], partner)),
    )

    wait_tile(0)
    raw[...] = multiply(0).astype(BF16)
    fetch_q(3)

    def project(n, carry):
        @pl.when(n == 2)
        def _():
            for rel in range(1, 4):
                new_copy(rel, 0).start()
            for c in new_outs[0]:
                c.start()

        @pl.when((n >= 3) & (n < 3 + 3 * parts))
        def _():
            e = n - 2
            q_copy((e + parts - 1) // parts, (e + parts - 1) % parts).start()

        @pl.when(n == 3 + 3 * parts)
        def _():
            for p in range(2, 8):
                for kind in range(2):
                    kv_copy(p, kind).start()

        wait_tile(n)
        rotate(n - 1)
        raw[...] = multiply(n).astype(BF16)

        @pl.when(n + WBUFS <= q_tiles)
        def _():
            fetch_q(n + WBUFS)

        @pl.when(n + WBUFS == q_tiles + 1)
        def _():
            fetch_kv(wv_in, q_tiles + 1)

        @pl.when(n + WBUFS >= p1_tiles)
        def _():
            fetch_o(n + WBUFS - p1_tiles)

        return carry

    lax.fori_loop(1, p1_tiles, project, 0)

    here = pl.ds(pl.multiple_of(8 * seg + chip * pair, pair), pair)
    for a in range(4):
        vstage[a] = raw[:, a * HEAD_DIM:(a + 1) * HEAD_DIM].astype(F32).T.astype(BF16)
    kbuf[here, :] = stage[0, :, pl.ds(pl.multiple_of((parts - 1) * TILE + chip * HEAD_DIM, HEAD_DIM), HEAD_DIM)]
    vbuf[:, here] = vstage[chip]

    def init(t, carry):
        peak_ref[t] = jnp.full((1, TILE), neg, F32)
        sum_ref[t] = jnp.zeros((1, TILE), F32)
        acc[t] = jnp.zeros((HEAD_DIM, TILE), F32)
        return carry

    lax.fori_loop(0, tiles, init, 0)
    for rel in range(1, 4):
        new_copy(rel, 1).start()
    for c in new_outs[1]:
        c.start()

    def place(t):
        rel, rest = t // per_chip, t % per_chip
        return rel, pl.ds(pl.multiple_of((rest % 2) * rows, rows), rows), rest // 2

    def q_tile(t):
        rel, some_rows, part = place(t)
        block = qbuf[rel, some_rows, pl.ds(pl.multiple_of(part * TILE, TILE), TILE)]
        return jnp.concatenate([block[:, h * HEAD_DIM:(h + 1) * HEAD_DIM] for h in range(HEADS)], axis=0)

    def step(pv=None, qk=None):
        if pv is not None:
            t, base, keys_p = pv
            old = peak_ref[t]
            top = jnp.maximum(old, jnp.max(chunk_max[...], axis=0, keepdims=True) * coef)
            fade = jnp.exp2(old - top)
            peak_ref[t] = top
        if qk is not None:
            tq, base_q, keys_q, has_new = qk
            q = q_tile(tq)
            first_row = flip_chip(chip, tq // per_chip) * pair + (tq % 2) * rows
        total = None
        values = None
        peaks = None
        for s in range(max(pv[2] if pv else 0, qk[2] if qk else 0) // SUB):
            lines = slice(s * SUB, (s + 1) * SUB)
            if pv is not None and s * SUB < keys_p:
                w = jnp.exp2(scores[lines, :] * coef - top)
                part = jnp.sum(w.reshape(SUB // 8, 8, TILE), axis=0)
                total = part if total is None else total + part
                v_part = vbuf[:, pl.ds(pl.multiple_of(base + s * SUB, SUB), SUB)]
                o_part = jnp.dot(v_part, w.astype(BF16), preferred_element_type=F32)
                values = o_part if values is None else values + o_part
            if qk is not None and s * SUB < keys_q:
                k_part = kbuf[pl.ds(pl.multiple_of(base_q + s * SUB, SUB), SUB), :]
                sc = lax.dot_general(k_part, q, (((1,), (1,)), ((), ())), preferred_element_type=F32)
                if has_new and s * SUB >= keys_a:
                    key = lax.broadcasted_iota(jnp.int32, (SUB, TILE), 0) + (s * SUB - keys_a)
                    row = lax.broadcasted_iota(jnp.int32, (SUB, TILE), 1) % rows + first_row
                    sc = jnp.where(key <= row, sc, neg)
                scores[lines, :] = sc
                part = jnp.max(sc.reshape(SUB // 8, 8, TILE), axis=0)
                peaks = part if peaks is None else jnp.maximum(peaks, part)
        if qk is not None:
            chunk_max[...] = peaks
        if pv is None:
            return None
        sums = sum_ref[t] * fade + jnp.sum(total, axis=0, keepdims=True)
        return sums, acc[t] * fade + values

    def keep(t, result):
        sum_ref[t], acc[t] = result

    def finish(t, result):
        sums, whole = result
        done = whole / sums
        rel, some_rows, part = place(t)
        done = jnp.concatenate([done[:, h * rows:(h + 1) * rows].T.astype(BF16) for h in range(HEADS)], axis=1)
        stage[rel, some_rows, pl.ds(pl.multiple_of(part * TILE, TILE), TILE)] = done
        hbuf[some_rows, pl.ds(pl.multiple_of(chip * width + part * TILE, TILE), TILE)] = done

    kv_wait(0)
    kv_wait(1)
    step(qk=(0, 0, keys_a, False))
    steps_a = 3 * tiles

    def body_a(i, carry):
        nxt = i + 1

        @pl.when((nxt >= per_chip) & (nxt < tiles) & (nxt % 2 == 0))
        def _():
            q_copy(nxt // per_chip, (nxt % per_chip) // 2).wait_recv()

        for v in (1, 2):
            @pl.when(nxt == v * tiles)
            def _():
                kv_wait(2 * v)
                kv_wait(2 * v + 1)
        t = i % tiles
        keep(t, step(pv=(t, (i // tiles) * keys_a, keys_a),
                     qk=(nxt % tiles, (nxt // tiles) * keys_a, keys_a, False)))
        return carry

    lax.fori_loop(0, steps_a - 1, body_a, 0)

    kv_wait(6)
    kv_wait(7)
    for rel in range(1, 4):
        new_copy(rel, 0).wait_recv()
        new_copy(rel, 1).wait_recv()
        new_copy(rel, 0).wait_send()
        for part in range(parts):
            q_copy(rel, part).wait_send()
    new_outs[0][0].wait()
    new_outs[0][1].wait_send()

    def tile_b(i):
        return (3 - i // per_chip) * per_chip + i % per_chip

    def o_copy(rel, part):
        cols = pl.ds(pl.multiple_of(part * TILE, TILE), TILE)
        there = pl.ds(pl.multiple_of(chip * width + part * TILE, TILE), TILE)
        return remote(stage.at[rel, :, cols], hbuf.at[:, there], osend.at[rel, part], orecv.at[rel, part],
                      2 * flip_chip(chip, rel) + core)

    def o_arrival(rel, part):
        there = pl.ds(pl.multiple_of(flip_chip(chip, rel) * width + part * TILE, TILE), TILE)
        return remote(hbuf.at[:, there], hbuf.at[:, there], osend.at[rel, part], orecv.at[rel, part],
                      2 * flip_chip(chip, rel) + core)

    last_t = tiles - 1
    base_b = 3 * keys_a
    keep(last_t, step(pv=(last_t, 2 * keys_a, keys_a), qk=(tile_b(0), base_b, keys_b, True)))

    def body_b(i, carry):
        @pl.when((i >= 2) & (i % 2 == 0) & (i <= 3 * per_chip))
        def _():
            done = i - 2
            o_copy(3 - done // per_chip, (done % per_chip) // 2).start()

        t = tile_b(i)
        finish(t, step(pv=(t, base_b, keys_b), qk=(tile_b(i + 1), base_b, keys_b, True)))
        return carry

    lax.fori_loop(0, tiles - 1, body_b, 0)
    finish(per_chip - 1, step(pv=(per_chip - 1, base_b, keys_b)))

    pl.semaphore_signal(free_sem, inc=1, device_id=device(partner), device_id_type=MESH)
    for rel in range(1, 4):
        for part in range(parts):
            o_arrival(rel, part).wait_recv()
    pl.semaphore_wait(free_sem, 1)

    sent, got, own = 0, out_tiles * rows, 2 * out_tiles * rows

    def lines(first, m):
        return pl.ds(pl.multiple_of(first + m * rows, rows), rows)

    def p_copy(m):
        return remote(scores.at[lines(sent, m), :], scores.at[lines(got, m), :], psend.at[m], precv.at[m], partner)

    def out_copy(m):
        cols = pl.ds(pl.multiple_of(m * TILE, TILE), TILE)
        return pltpu.make_async_copy(outst.at[:, cols], out.at[:, cols], outsem.at[m])

    def combine(m):
        p_copy(m).wait_recv()
        cols = pl.ds(pl.multiple_of(m * TILE, TILE), TILE)
        both = scores[lines(own, m), :] + scores[lines(got, m), :]
        outst[:, cols] = (xbuf[my_rows, cols].astype(F32) + both).astype(BF16)
        out_copy(m).start()

    def output(m, carry):
        @pl.when(m >= 1)
        def _():
            p_copy(m - 1).start()

        @pl.when(m >= 2)
        def _():
            combine(m - 2)

        wait_tile(p1_tiles + m)
        both = multiply(p1_tiles + m)
        scores[lines(own, m), :] = jnp.where(core == 0, both[:rows], both[rows:])
        scores[lines(sent, m), :] = jnp.where(core == 0, both[rows:], both[:rows])

        @pl.when(m + WBUFS < out_tiles)
        def _():
            fetch_o(m + WBUFS)

        return carry

    lax.fori_loop(0, out_tiles, output, 0)
    p_copy(out_tiles - 1).start()
    combine(out_tiles - 2)
    combine(out_tiles - 1)

    def drain(m, carry):
        p_copy(m).wait_send()
        out_copy(m).wait()
        return carry

    lax.fori_loop(0, out_tiles, drain, 0)
    x_remote.wait_send()
    for p in range(1, 8):
        for kind in range(2):
            kv_copy(p, kind).wait_send()
    for rel in range(1, 4):
        new_copy(rel, 1).wait_send()
        for part in range(parts):
            o_copy(rel, part).wait_send()
    new_outs[0][1].wait_recv()
    new_outs[1][0].wait()
    new_outs[1][1].wait()


def block(x, kt, vt, ln, gains, cos_tab, sin_tab, w_q, w_k, w_v, w_o):
    rows, hid = x.shape
    _, seg, _ = kt.shape
    width = w_q.shape[1] // 8
    pair, new = 2 * rows, 8 * rows
    parts = width // TILE
    tiles = 8 * parts
    out_tiles = hid // TILE
    keys_b = 2 * seg + new
    flops = 4 * (8 * seg + new) * 8 * rows * width + 8 * rows * hid * width * 2
    hbm = pl.BlockSpec(memory_space=pl.ANY)
    vmem = pl.BlockSpec(memory_space=pltpu.VMEM)
    dma = pltpu.SemaphoreType.DMA
    return pl.pallas_call(
        functools.partial(block_kernel, rows, seg, width),
        out_shape=(
            jax.ShapeDtypeStruct((rows, hid), BF16),
            jax.ShapeDtypeStruct((2, rows, TILE), BF16),
            jax.ShapeDtypeStruct((2, rows, TILE), BF16),
        ),
        in_specs=[hbm, hbm, hbm, vmem, vmem, vmem, vmem, hbm, hbm, hbm, hbm],
        out_specs=(hbm, hbm, hbm),
        scratch_shapes=[
            pltpu.VMEM((pair, hid), BF16),
            pltpu.VMEM((pair, hid), BF16),
            pltpu.VMEM((WBUFS, hid, TILE), BF16),
            pltpu.VMEM((pair, TILE), BF16),
            pltpu.VMEM((5, pair, width), BF16),
            pltpu.VMEM((4, HEAD_DIM, pair), BF16),
            pltpu.VMEM((4, pair, width), BF16),
            pltpu.VMEM((8 * seg + new, HEAD_DIM), BF16),
            pltpu.VMEM((HEAD_DIM, 8 * seg + new), BF16),
            pltpu.VMEM((max(keys_b, 3 * out_tiles * rows), TILE), F32),
            pltpu.VMEM((tiles, HEAD_DIM, TILE), F32),
            pltpu.VMEM((tiles, 1, TILE), F32),
            pltpu.VMEM((tiles, 1, TILE), F32),
            pltpu.VMEM((8, TILE), F32),
            pltpu.VMEM((rows, hid), BF16),
            dma((WBUFS, 4)),
            dma((3,)),
            dma((4, parts)), dma((4, parts)),
            dma((2, 8)), dma((2, 8)),
            dma((2, 4)), dma((2, 4)),
            dma((4, parts)), dma((4, parts)),
            dma((2,)), dma((4,)),
            dma((out_tiles,)), dma((out_tiles,)),
            dma((out_tiles,)),
            pltpu.SemaphoreType.REGULAR,
        ],
        compiler_params=pltpu.CompilerParams(
            collective_id=0, has_side_effects=True, vmem_limit_bytes=67043328),
        cost_estimate=pl.CostEstimate(flops=flops, bytes_accessed=200 * 1024 * 1024, transcendentals=flops // 512),
        name="block",
    )(x, kt, vt, ln, gains, cos_tab, sin_tab, w_q, w_k, w_v, w_o)


def solution(mesh):
    cp_size = mesh.shape['cp']
    row_spec = P(('dp', 'cp'), None)
    cache_spec = P(('dp', 'cp'), None, None)
    whole = P()

    def device_step(x_rows, k_cache, v_cache, ln_gain, w_q, w_k, w_v, w_o, q_gain, k_gain):
        rows = x_rows.shape[0]
        prefix_len = k_cache.shape[0] * cp_size
        chip = lax.axis_index('cp') // 2
        positions = (prefix_len + chip * 2 * rows + jnp.arange(2 * rows)).astype(F32)
        half = HEAD_DIM // 2
        inv_freq = ROPE_THETA ** (-jnp.arange(half, dtype=F32) * (2.0 / HEAD_DIM))
        angles = positions[:, None] * inv_freq[None, :]
        cos_half, sin_half = jnp.cos(angles), jnp.sin(angles)
        cos_tab = jnp.concatenate([cos_half, cos_half], axis=1)
        sin_tab = jnp.concatenate([-sin_half, sin_half], axis=1)
        gains = jnp.stack([k_gain, q_gain]).astype(F32)[:, None, :]
        out, k_pairs, v_pairs = block(
            x_rows,
            jnp.transpose(k_cache, (1, 0, 2)),
            jnp.transpose(v_cache, (1, 2, 0)),
            ln_gain.astype(F32)[None, :], gains, cos_tab, sin_tab, w_q, w_k, w_v, w_o)

        def heads(pairs):
            return jnp.transpose(pairs.reshape(2, rows, 4, HEAD_DIM), (1, 2, 0, 3)).reshape(rows, 8, HEAD_DIM)

        return out, heads(k_pairs), heads(v_pairs)

    return jax.shard_map(device_step, mesh=mesh, in_specs=(row_spec, cache_spec, cache_spec, whole, whole, whole, whole, whole, whole, whole), out_specs=(row_spec, cache_spec, cache_spec), check_vma=False)
```

```python
import functools
import math

import jax
import jax.numpy as jnp
from jax import lax
from jax.experimental import pallas as pl
from jax.experimental.pallas import tpu as pltpu
from jax.sharding import PartitionSpec as P

HEAD_DIM = 128
ROPE_THETA = 1.0e6
NORM_EPS = 1.0e-6
MESH = pl.DeviceIdType.MESH
F32 = jnp.float32
BF16 = jnp.bfloat16

ORD = (0, 1, 2, 4, 3, 5, 6, 7)
SUB = 256
TILE = 512
HEADS = TILE // HEAD_DIM
WBUFS = 3


def div(a, b):
    return a // b if isinstance(a, int) else lax.div(a, jnp.int32(b))


def rem(a, b):
    return a % b if isinstance(a, int) else lax.rem(a, jnp.int32(b))


def flip(me, rel):
    out = 0
    for bit in (1, 2, 4):
        mine = rem(div(me, bit), 2)
        out = out + bit * ((1 - mine) if rel & bit else mine)
    return out


def flip_chip(chip, rel):
    return rem(rem(chip, 2) + rem(rel, 2), 2) + 2 * rem(div(chip, 2) + div(rel, 2), 2)


def block_kernel(rows, seg, width,
                 x_in, k_in, v_in, ln_in, gain_in, cos_in, sin_in, wq_in, wk_in, wv_in, wo_in,
                 out, k_out, v_out, kt, vt,
                 xres, hbuf, wbuf, raw, stage, vstage, qbuf, kbuf, vbuf, scores, acc, kraw, vraw, kturn, vturn, peak_ref, sum_ref, fade_ref, chunk_max, ahead_ref, outst,
                 wsem, xsem, qsend, qrecv, kvsend, kvrecv, nsend, nrecv, osend, orecv, ksend, krecv, psend, precv, outsem, turnsem,
                 free_sem):
    dp = lax.axis_index("dp")
    me = lax.axis_index("cp")
    chip, core = div(me, 2), rem(me, 2)
    hid = wbuf.shape[1]
    pair = 2 * rows
    new = 8 * rows
    parts = width // TILE
    per_chip = 2 * parts
    tiles = 4 * per_chip
    keys_a = 2 * seg
    keys_b = 2 * seg + new
    coef = math.log2(math.e) * HEAD_DIM ** -0.5
    neg = float("-inf")
    q_tiles = 4 * parts
    p1_tiles = q_tiles + 2
    out_tiles = hid // TILE
    chunk = hid // 4
    turns = 8
    depth = seg // turns

    def device(index):
        return (dp, index)

    partner = flip(me, 1)

    barrier = pltpu.get_barrier_semaphore()
    for rel in range(1, 8):
        pl.semaphore_signal(barrier, inc=1, device_id=device(flip(me, rel)), device_id_type=MESH)

    def remote(src, dst, send, recv, index):
        return pltpu.make_async_remote_copy(
            src_ref=src, dst_ref=dst, send_sem=send, recv_sem=recv, device_id=device(index), device_id_type=MESH)

    my_rows = pl.ds(pl.multiple_of(core * rows, rows), rows)
    other_rows = pl.ds(pl.multiple_of((1 - core) * rows, rows), rows)

    def tile_of(ref, slot, a):
        return ref.at[slot, pl.ds(a * chunk, chunk), :]

    def fetch_kv(ref, n):
        slot = rem(n, WBUFS)
        for a in range(4):
            first = pl.multiple_of((2 * a + core) * HEAD_DIM, HEAD_DIM)
            pltpu.make_async_copy(ref.at[:, pl.ds(first, HEAD_DIM)],
                                  wbuf.at[slot, :, pl.ds(a * HEAD_DIM, HEAD_DIM)], wsem.at[slot, a]).start()

    def fetch_q(n):
        slot = rem(n, WBUFS)
        g, part = div(n - 1, parts), rem(n - 1, parts)
        head = 2 * flip_chip(chip, rem(g + 1, 4)) + core
        first = pl.multiple_of(head * width + part * TILE, TILE)
        for a in range(4):
            pltpu.make_async_copy(wq_in.at[pl.ds(a * chunk, chunk), pl.ds(first, TILE)],
                                  tile_of(wbuf, slot, a), wsem.at[slot, a]).start()

    def fetch_o(m):
        slot = rem(p1_tiles + m, WBUFS)
        first = pl.multiple_of(m * TILE, TILE)
        for a in range(4):
            top = pl.multiple_of((2 * a + core) * width, width)
            pltpu.make_async_copy(wo_in.at[pl.ds(top, width), pl.ds(first, TILE)],
                                  tile_of(wbuf, slot, a), wsem.at[slot, a]).start()

    def wait_tile(n):
        slot = rem(n, WBUFS)
        for a in range(4):
            pltpu.make_async_copy(tile_of(wbuf, slot, a), tile_of(wbuf, slot, a), wsem.at[slot, a]).wait()

    x_local = pltpu.make_async_copy(x_in, hbuf.at[my_rows, :], xsem.at[0])
    x_remote = remote(x_in, hbuf.at[my_rows, :], xsem.at[1], xsem.at[2], partner)
    x_local.start()
    fetch_kv(wk_in, 0)
    pl.semaphore_wait(barrier, 7)
    x_remote.start()
    fetch_q(1)
    fetch_q(2)

    def kv_copy(p, kind):
        peer = flip(me, ORD[p])
        if kind == 0:
            src, dst = kt.at[peer], kbuf.at[pl.ds(p * seg, seg), :]
        else:
            src, dst = vt.at[peer], vbuf.at[:, pl.ds(p * seg, seg)]
        if p == 0:
            return pltpu.make_async_copy(src, dst, kvrecv.at[kind, 0])
        return remote(src, dst, kvsend.at[kind, p], kvrecv.at[kind, p], peer)

    def kv_send(pair_index):
        for p in (2 * pair_index, 2 * pair_index + 1):
            for kind in range(2):
                kv_copy(p, kind).start()

    def kv_wait(p):
        for kind in range(2):
            if p == 0:
                kv_copy(p, kind).wait()
            else:
                kv_copy(p, kind).wait_recv()

    def turn_in(c):
        where = pl.ds(pl.multiple_of(c * depth, depth), depth)
        slot = rem(c, 2)
        return (pltpu.make_async_copy(k_in.at[where], kraw.at[slot], turnsem.at[0, slot]),
                pltpu.make_async_copy(v_in.at[where], vraw.at[slot], turnsem.at[1, slot]))

    def turn_out(c):
        where = pl.ds(pl.multiple_of(c * depth, depth), depth)
        return (pltpu.make_async_copy(kturn, kt.at[:, where, :], turnsem.at[2, 0]),
                pltpu.make_async_copy(vturn, vt.at[:, :, where], turnsem.at[2, 1]))

    def turn(c):
        slot = rem(c, 2)
        acc[pl.ds(0, 8 * depth), :] = kraw[slot].astype(F32).reshape(8 * depth, HEAD_DIM)
        acc[pl.ds(8 * depth, 8 * depth), :] = vraw[slot].astype(F32).reshape(8 * depth, HEAD_DIM)
        for h in range(8):
            kturn[h] = acc[pl.ds(h, depth, stride=8), :].astype(BF16)
            vturn[h] = acc[pl.ds(8 * depth + h, depth, stride=8), :].T.astype(BF16)

    for c in turn_in(0):
        c.start()

    def normalise(first_row):
        def some(i, carry):
            at = pl.multiple_of(first_row + i * 32, 32)
            wide = hbuf[pl.ds(at, 32), :].astype(F32)
            mean_sq = jnp.sum(wide * wide, axis=-1, keepdims=True) * (1.0 / hid)
            hbuf[pl.ds(at, 32), :] = (wide * lax.rsqrt(mean_sq + NORM_EPS) * ln_in[...]).astype(BF16)
            return carry
        lax.fori_loop(0, rows // 32, some, 0)

    x_local.wait()
    normalise(core * rows)
    x_remote.wait_recv()
    normalise((1 - core) * rows)

    def multiply(n):
        slot = rem(n, WBUFS)
        return jnp.dot(hbuf[...], wbuf[slot], preferred_element_type=F32)

    def rotate(e):
        group, part = div(e + parts - 1, parts), rem(e + parts - 1, parts)
        gain = gain_in[jnp.minimum(e, 1)]
        cos_tab, sin_tab = cos_in[...], sin_in[...]
        done = []
        for h in range(HEADS):
            vals = raw[:, h * HEAD_DIM:(h + 1) * HEAD_DIM].astype(F32)
            mean_sq = jnp.sum(vals * vals, axis=-1, keepdims=True) * (1.0 / HEAD_DIM)
            vals = vals * lax.rsqrt(mean_sq + NORM_EPS) * gain
            done.append((vals * cos_tab + pltpu.roll(vals, HEAD_DIM // 2, 1) * sin_tab).astype(BF16))
        done = jnp.concatenate(done, axis=1)
        where = pl.ds(pl.multiple_of(part * TILE, TILE), TILE)
        stage[group, :, where] = done
        qbuf[0, :, where] = done

    def q_copy(rel, part):
        cols = pl.ds(pl.multiple_of(part * TILE, TILE), TILE)
        return remote(stage.at[rel, :, cols], qbuf.at[rel, :, cols], qsend.at[rel, part], qrecv.at[rel, part],
                      2 * flip_chip(chip, rel) + core)

    def new_copy(rel, kind):
        other = flip_chip(chip, rel)
        here = pl.ds(pl.multiple_of(8 * seg + chip * pair, pair), pair)
        if kind == 0:
            first = pl.multiple_of((parts - 1) * TILE + other * HEAD_DIM, HEAD_DIM)
            src, dst = stage.at[0, :, pl.ds(first, HEAD_DIM)], kbuf.at[here, :]
        else:
            src, dst = vstage.at[other], vbuf.at[:, here]
        return remote(src, dst, nsend.at[kind, rel], nrecv.at[kind, rel], 2 * other + core)

    def new_outs(kind):
        copies = []
        for a in range(4):
            if kind == 0:
                src, cols = stage.at[0], pl.ds((parts - 1) * TILE + a * HEAD_DIM, HEAD_DIM)
            else:
                src, cols = raw, pl.ds(a * HEAD_DIM, HEAD_DIM)
            dst = (k_out, v_out)[kind].at[2 * a + core]
            copies.append((
                pltpu.make_async_copy(src.at[my_rows, cols], dst, krecv.at[kind, 0, a]),
                remote(src.at[other_rows, cols], dst, ksend.at[kind, a], krecv.at[kind, 1, a], partner)))
        return copies

    def out_arrival(kind, a):
        dst = (k_out, v_out)[kind].at[2 * a + 1 - core]
        return remote(dst, dst, ksend.at[kind, a], krecv.at[kind, 1, a], partner)

    wait_tile(0)
    raw[...] = multiply(0).astype(BF16)
    fetch_q(3)

    def project(turning, n, carry):
        @pl.when(n == 2)
        def _():
            for rel in range(1, 4):
                new_copy(rel, 0).start()
            for here_copy, there_copy in new_outs(0):
                here_copy.start()
                there_copy.start()

        @pl.when((n >= 3) & (n < 3 + 3 * parts))
        def _():
            e = n - 2
            q_copy(div(e + parts - 1, parts), rem(e + parts - 1, parts)).start()

        if turning:
            @pl.when(n < turns)
            def _():
                for c in turn_in(n):
                    c.start()

            for c in turn_in(n - 1):
                c.wait()

            @pl.when(n >= 2)
            def _():
                for c in turn_out(n - 2):
                    c.wait()
        else:
            @pl.when(n == turns + 1)
            def _():
                for c in turn_out(turns - 1):
                    c.wait()
                for p in range(2):
                    for kind in range(2):
                        kv_copy(p, kind).start()

            @pl.when(n == 3 + 3 * parts)
            def _():
                kv_send(1)

        wait_tile(n)
        rotate(n - 1)
        if turning:
            turn(n - 1)
        raw[...] = multiply(n).astype(BF16)
        if turning:
            for c in turn_out(n - 1):
                c.start()

        @pl.when(n + WBUFS <= q_tiles)
        def _():
            fetch_q(n + WBUFS)

        @pl.when(n + WBUFS == q_tiles + 1)
        def _():
            fetch_kv(wv_in, q_tiles + 1)

        @pl.when((n + WBUFS >= p1_tiles) & (n + WBUFS < p1_tiles + WBUFS - 1))
        def _():
            fetch_o(n + WBUFS - p1_tiles)

        return carry

    lax.fori_loop(1, turns + 1, functools.partial(project, True), 0)
    lax.fori_loop(turns + 1, p1_tiles, functools.partial(project, False), 0)

    here = pl.ds(pl.multiple_of(8 * seg + chip * pair, pair), pair)
    for a in range(4):
        vstage[a] = raw[:, a * HEAD_DIM:(a + 1) * HEAD_DIM].astype(F32).T.astype(BF16)
    kbuf[here, :] = stage[0, :, pl.ds(pl.multiple_of((parts - 1) * TILE + chip * HEAD_DIM, HEAD_DIM), HEAD_DIM)]
    vbuf[:, here] = vstage[chip]

    def acc_rows(t, h):
        return pl.ds(pl.multiple_of((t * HEADS + h) * HEAD_DIM, HEAD_DIM), HEAD_DIM)

    def init(t, carry):
        peak_ref[t] = jnp.full((1, TILE), neg, F32)
        sum_ref[t] = jnp.zeros((1, TILE), F32)
        for h in range(HEADS):
            acc[acc_rows(t, h), :] = jnp.zeros((HEAD_DIM, rows), F32)
        return carry

    lax.fori_loop(0, tiles, init, 0)
    ahead_ref[...] = (lax.broadcasted_iota(jnp.int32, (SUB, rows), 0)
                      - lax.broadcasted_iota(jnp.int32, (SUB, rows), 1))
    for rel in range(1, 4):
        new_copy(rel, 1).start()
    for here_copy, there_copy in new_outs(1):
        here_copy.start()
        there_copy.start()

    def place(t):
        rel, rest = div(t, per_chip), rem(t, per_chip)
        return rel, pl.ds(pl.multiple_of(rem(rest, 2) * rows, rows), rows), div(rest, 2)

    def q_tile(t):
        rel, some_rows, part = place(t)
        block = qbuf[rel, some_rows, pl.ds(pl.multiple_of(part * TILE, TILE), TILE)]
        return jnp.concatenate([block[:, h * HEAD_DIM:(h + 1) * HEAD_DIM] for h in range(HEADS)], axis=0)

    probs = wbuf.at[(p1_tiles + WBUFS - 1) % WBUFS]

    def step(pv=None, sm=None, qk=None, end=None):
        if end is not None:
            finish(end)
        if pv is not None:
            t_pv, base_pv, keys_pv = pv
            fade_pv = fade_ref[...]
        if sm is not None:
            t_sm, keys_sm = sm
            old = peak_ref[t_sm]
            top = jnp.maximum(old, jnp.max(chunk_max[...], axis=0, keepdims=True) * coef)
            fade = jnp.exp2(old - top)
            peak_ref[t_sm] = top
        if qk is not None:
            t_qk, base_qk, keys_qk, has_new = qk
            q = q_tile(t_qk)
            first_row = flip_chip(chip, div(t_qk, per_chip)) * pair + rem(t_qk, 2) * rows if has_new else None
        total = None
        values = None
        peaks = None
        most = max(pv[2] if pv else 0, sm[1] if sm else 0, qk[2] if qk else 0)
        for s in range(most // SUB):
            lines = slice(s * SUB, (s + 1) * SUB)
            if pv is not None and s * SUB < keys_pv:
                v_part = vbuf[:, pl.ds(pl.multiple_of(base_pv + s * SUB, SUB), SUB)]
                o_part = jnp.dot(v_part, probs[lines, :], preferred_element_type=F32)
                values = o_part if values is None else values + o_part
            if sm is not None and s * SUB < keys_sm:
                w = jnp.exp2(scores[lines, :] * coef - top)
                part = jnp.sum(w.reshape(SUB // 8, 8, TILE), axis=0)
                total = part if total is None else total + part
                probs[lines, :] = w.astype(BF16)
            if qk is not None and s * SUB < keys_qk:
                k_part = kbuf[pl.ds(pl.multiple_of(base_qk + s * SUB, SUB), SUB), :]
                sc = lax.dot_general(k_part, q, (((1,), (1,)), ((), ())), preferred_element_type=F32)
                if has_new and s * SUB >= keys_a:
                    seen = ahead_ref[...] <= first_row - (s * SUB - keys_a)
                    sc = jnp.concatenate(
                        [jnp.where(seen, sc[:, h * rows:(h + 1) * rows], neg) for h in range(HEADS)], axis=1)
                scores[lines, :] = sc
                part = jnp.max(sc.reshape(SUB // 8, 8, TILE), axis=0)
                peaks = part if peaks is None else jnp.maximum(peaks, part)
        if qk is not None:
            chunk_max[...] = peaks
        if sm is not None:
            sum_ref[t_sm] = sum_ref[t_sm] * fade + jnp.sum(total, axis=0, keepdims=True)
            fade_ref[...] = fade
        if pv is not None:
            for h in range(HEADS):
                cols = slice(h * rows, (h + 1) * rows)
                acc[acc_rows(t_pv, h), :] = acc[acc_rows(t_pv, h), :] * fade_pv[:, cols] + values[:, cols]

    def finish(t):
        sums = sum_ref[t]
        rel, some_rows, part = place(t)
        done = jnp.concatenate(
            [(acc[acc_rows(t, h), :] / sums[:, h * rows:(h + 1) * rows]).T.astype(BF16) for h in range(HEADS)], axis=1)
        stage[rel, some_rows, pl.ds(pl.multiple_of(part * TILE, TILE), TILE)] = done
        hbuf[some_rows, pl.ds(pl.multiple_of(chip * width + part * TILE, TILE), TILE)] = done

    steps_a = 3 * tiles

    def item_a(i):
        return rem(i, tiles), div(i, tiles) * keys_a, keys_a

    kv_wait(0)
    kv_wait(1)
    step(qk=(*item_a(0), False))
    step(sm=(0, keys_a), qk=(*item_a(1), False))

    def body_a(i, carry):
        nxt = i + 1

        @pl.when((nxt >= per_chip) & (nxt < tiles) & (rem(nxt, 2) == 0))
        def _():
            q_copy(div(nxt, per_chip), div(rem(nxt, per_chip), 2)).wait_recv()

        @pl.when(nxt == 2 * tiles // 3)
        def _():
            kv_send(2)

        @pl.when(nxt == 4 * tiles // 3)
        def _():
            kv_send(3)

        for v in (1, 2):
            @pl.when(nxt == v * tiles)
            def _():
                kv_wait(2 * v)
                kv_wait(2 * v + 1)
        step(pv=item_a(i - 1), sm=(rem(i, tiles), keys_a), qk=(*item_a(nxt), False))
        return carry

    lax.fori_loop(1, steps_a - 1, body_a, 0)

    kv_wait(6)
    kv_wait(7)
    for rel in range(1, 4):
        new_copy(rel, 0).wait_recv()
        new_copy(rel, 1).wait_recv()
        new_copy(rel, 0).wait_send()
        for part in range(parts):
            q_copy(rel, part).wait_send()
    for here_copy, there_copy in new_outs(0):
        here_copy.wait()
        there_copy.wait_send()

    def tile_b(i):
        return (3 - div(i, per_chip)) * per_chip + rem(i, per_chip)

    def o_copy(rel, part):
        cols = pl.ds(pl.multiple_of(part * TILE, TILE), TILE)
        there = pl.ds(pl.multiple_of(chip * width + part * TILE, TILE), TILE)
        return remote(stage.at[rel, :, cols], hbuf.at[:, there], osend.at[rel, part], orecv.at[rel, part],
                      2 * flip_chip(chip, rel) + core)

    def o_arrival(rel, part):
        there = pl.ds(pl.multiple_of(flip_chip(chip, rel) * width + part * TILE, TILE), TILE)
        return remote(hbuf.at[:, there], hbuf.at[:, there], osend.at[rel, part], orecv.at[rel, part],
                      2 * flip_chip(chip, rel) + core)

    base_b = 3 * keys_a

    def item_b(i):
        return tile_b(i), base_b, keys_b

    step(pv=item_a(steps_a - 2), sm=((steps_a - 1) % tiles, keys_a), qk=(*item_b(0), True))
    step(pv=item_a(steps_a - 1), sm=(tile_b(0), keys_b), qk=(*item_b(1), True))
    step(pv=item_b(0), sm=(tile_b(1), keys_b), qk=(*item_b(2), True))

    def body_b(i, carry):
        @pl.when((i >= 4) & (rem(i, 2) == 0) & (i <= 3 * per_chip + 2))
        def _():
            done = i - 4
            o_copy(3 - div(done, per_chip), div(rem(done, per_chip), 2)).start()

        step(pv=item_b(i - 1), sm=(tile_b(i), keys_b), qk=(*item_b(i + 1), True), end=tile_b(i - 2))
        return carry

    lax.fori_loop(2, tiles - 1, body_b, 0)
    step(pv=item_b(tiles - 2), sm=(tile_b(tiles - 1), keys_b), end=tile_b(tiles - 3))
    step(pv=item_b(tiles - 1), end=tile_b(tiles - 2))
    finish(tile_b(tiles - 1))
    fetch_o(WBUFS - 1)

    pl.semaphore_signal(free_sem, inc=1, device_id=device(partner), device_id_type=MESH)
    for rel in range(1, 4):
        for part in range(parts):
            o_arrival(rel, part).wait_recv()
    pl.semaphore_wait(free_sem, 1)

    sent, got, own = 0, out_tiles * rows, 2 * out_tiles * rows

    def lines(first, m):
        return pl.ds(pl.multiple_of(first + m * rows, rows), rows)

    def p_copy(m):
        return remote(scores.at[lines(sent, m), :], scores.at[lines(got, m), :], psend.at[m], precv.at[m], partner)

    def out_copy(m):
        cols = pl.ds(pl.multiple_of(m * TILE, TILE), TILE)
        return pltpu.make_async_copy(outst.at[rem(m, 2)], out.at[:, cols], outsem.at[m])

    def x_copy(m):
        cols = pl.ds(pl.multiple_of(m * TILE, TILE), TILE)
        return pltpu.make_async_copy(x_in.at[:, cols], xres.at[rem(m, 2)], xsem.at[3 + rem(m, 2)])

    def combine(m):
        if isinstance(m, int):
            out_copy(m - 2).wait()
        else:
            @pl.when(m >= 2)
            def _():
                out_copy(m - 2).wait()
        p_copy(m).wait_recv()
        x_copy(m).wait()
        both = scores[lines(own, m), :] + scores[lines(got, m), :]
        outst[rem(m, 2)] = (xres[rem(m, 2)].astype(F32) + both).astype(BF16)
        out_copy(m).start()

    def output(m, carry):
        @pl.when(m >= 1)
        def _():
            p_copy(m - 1).start()

        @pl.when(m >= 2)
        def _():
            combine(m - 2)

        x_copy(m).start()
        wait_tile(p1_tiles + m)
        both = multiply(p1_tiles + m)
        scores[lines(own, m), :] = jnp.where(core == 0, both[:rows], both[rows:])
        scores[lines(sent, m), :] = jnp.where(core == 0, both[rows:], both[:rows])

        @pl.when(m + WBUFS < out_tiles)
        def _():
            fetch_o(m + WBUFS)

        return carry

    lax.fori_loop(0, out_tiles, output, 0)
    p_copy(out_tiles - 1).start()
    combine(out_tiles - 2)
    combine(out_tiles - 1)

    def drain(m, carry):
        p_copy(m).wait_send()
        return carry

    lax.fori_loop(0, out_tiles, drain, 0)
    out_copy(out_tiles - 2).wait()
    out_copy(out_tiles - 1).wait()
    x_remote.wait_send()
    for p in range(1, 8):
        for kind in range(2):
            kv_copy(p, kind).wait_send()
    for rel in range(1, 4):
        new_copy(rel, 1).wait_send()
        for part in range(parts):
            o_copy(rel, part).wait_send()
    for here_copy, there_copy in new_outs(1):
        here_copy.wait()
        there_copy.wait_send()
    for a in range(4):
        out_arrival(0, a).wait_recv()
        out_arrival(1, a).wait_recv()


def block(x, k_cache, v_cache, ln, gains, cos_tab, sin_tab, w_q, w_k, w_v, w_o):
    rows, hid = x.shape
    seg = k_cache.shape[0]
    width = w_q.shape[1] // 8
    pair, new = 2 * rows, 8 * rows
    parts = width // TILE
    tiles = 8 * parts
    out_tiles = hid // TILE
    keys_b = 2 * seg + new
    flops = 4 * (8 * seg + new) * 8 * rows * width + 8 * rows * hid * width * 2
    hbm = pl.BlockSpec(memory_space=pl.ANY)
    vmem = pl.BlockSpec(memory_space=pltpu.VMEM)
    dma = pltpu.SemaphoreType.DMA
    return pl.pallas_call(
        functools.partial(block_kernel, rows, seg, width),
        out_shape=(
            jax.ShapeDtypeStruct((rows, hid), BF16),
            jax.ShapeDtypeStruct((8, rows, HEAD_DIM), BF16),
            jax.ShapeDtypeStruct((8, rows, HEAD_DIM), BF16),
            jax.ShapeDtypeStruct((8, seg, HEAD_DIM), BF16),
            jax.ShapeDtypeStruct((8, HEAD_DIM, seg), BF16),
        ),
        in_specs=[hbm, hbm, hbm, vmem, vmem, vmem, vmem, hbm, hbm, hbm, hbm],
        out_specs=(hbm,) * 5,
        scratch_shapes=[
            pltpu.VMEM((2, rows, TILE), BF16),
            pltpu.VMEM((pair, hid), BF16),
            pltpu.VMEM((WBUFS, hid, TILE), BF16),
            pltpu.VMEM((pair, TILE), BF16),
            pltpu.VMEM((5, pair, width), BF16),
            pltpu.VMEM((4, HEAD_DIM, pair), BF16),
            pltpu.VMEM((4, pair, width), BF16),
            pltpu.VMEM((8 * seg + new, HEAD_DIM), BF16),
            pltpu.VMEM((HEAD_DIM, 8 * seg + new), BF16),
            pltpu.VMEM((max(keys_b, 3 * out_tiles * rows), TILE), F32),
            pltpu.VMEM((tiles * HEADS * HEAD_DIM, rows), F32),
            pltpu.VMEM((2, seg // 8, 8, HEAD_DIM), BF16),
            pltpu.VMEM((2, seg // 8, 8, HEAD_DIM), BF16),
            pltpu.VMEM((8, seg // 8, HEAD_DIM), BF16),
            pltpu.VMEM((8, HEAD_DIM, seg // 8), BF16),
            pltpu.VMEM((tiles, 1, TILE), F32),
            pltpu.VMEM((tiles, 1, TILE), F32),
            pltpu.VMEM((1, TILE), F32),
            pltpu.VMEM((8, TILE), F32),
            pltpu.VMEM((SUB, rows), jnp.int32),
            pltpu.VMEM((2, rows, TILE), BF16),
            dma((WBUFS, 4)),
            dma((5,)),
            dma((4, parts)), dma((4, parts)),
            dma((2, 8)), dma((2, 8)),
            dma((2, 4)), dma((2, 4)),
            dma((4, parts)), dma((4, parts)),
            dma((2, 4)), dma((2, 2, 4)),
            dma((out_tiles,)), dma((out_tiles,)),
            dma((out_tiles,)),
            dma((3, 2)),
            pltpu.SemaphoreType.REGULAR,
        ],
        compiler_params=pltpu.CompilerParams(
            collective_id=0, has_side_effects=True, vmem_limit_bytes=67043328),
        cost_estimate=pl.CostEstimate(flops=flops, bytes_accessed=200 * 1024 * 1024, transcendentals=flops // 512),
        name="block",
    )(x, k_cache, v_cache, ln, gains, cos_tab, sin_tab, w_q, w_k, w_v, w_o)


def solution(mesh):
    cp_size = mesh.shape['cp']
    row_spec = P(('dp', 'cp'), None)
    cache_spec = P(('dp', 'cp'), None, None)
    whole = P()

    def device_step(x_rows, k_cache, v_cache, ln_gain, w_q, w_k, w_v, w_o, q_gain, k_gain):
        rows = x_rows.shape[0]
        prefix_len = k_cache.shape[0] * cp_size
        chip = lax.axis_index('cp') // 2
        positions = (prefix_len + chip * 2 * rows + jnp.arange(2 * rows)).astype(F32)
        half = HEAD_DIM // 2
        inv_freq = ROPE_THETA ** (-jnp.arange(half, dtype=F32) * (2.0 / HEAD_DIM))
        angles = positions[:, None] * inv_freq[None, :]
        cos_half, sin_half = jnp.cos(angles), jnp.sin(angles)
        cos_tab = jnp.concatenate([cos_half, cos_half], axis=1)
        sin_tab = jnp.concatenate([-sin_half, sin_half], axis=1)
        gains = jnp.stack([k_gain, q_gain]).astype(F32)[:, None, :]
        out, k_heads, v_heads, _, _ = block(
            x_rows, k_cache, v_cache, ln_gain.astype(F32)[None, :], gains, cos_tab, sin_tab, w_q, w_k, w_v, w_o)
        return out, jnp.transpose(k_heads, (1, 0, 2)), jnp.transpose(v_heads, (1, 0, 2))

    return jax.shard_map(device_step, mesh=mesh, in_specs=(row_spec, cache_spec, cache_spec, whole, whole, whole, whole, whole, whole, whole), out_specs=(row_spec, cache_spec, cache_spec), check_vma=False)
```

```python
import functools
import math

import jax
import jax.numpy as jnp
from jax import lax
from jax.experimental import pallas as pl
from jax.experimental.pallas import tpu as pltpu
from jax.sharding import PartitionSpec as P

HEAD_DIM = 128
ROPE_THETA = 1.0e6
NORM_EPS = 1.0e-6
MESH = pl.DeviceIdType.MESH
F32 = jnp.float32
BF16 = jnp.bfloat16

ORD = (0, 1, 2, 4, 3, 5, 6, 7)
SUB = 256
TILE = 512
HEADS = TILE // HEAD_DIM
WBUFS = 3


def div(a, b):
    return a // b if isinstance(a, int) else lax.div(a, jnp.int32(b))


def rem(a, b):
    return a % b if isinstance(a, int) else lax.rem(a, jnp.int32(b))


def flip(me, rel):
    out = 0
    for bit in (1, 2, 4):
        mine = rem(div(me, bit), 2)
        out = out + bit * ((1 - mine) if rel & bit else mine)
    return out


def flip_chip(chip, rel):
    return rem(rem(chip, 2) + rem(rel, 2), 2) + 2 * rem(div(chip, 2) + div(rel, 2), 2)


def block_kernel(rows, seg, width,
                 x_in, k_in, v_in, gain_in, cos_in, sin_in, wq_in, wk_in, wv_in, wo_in,
                 out, k_out, v_out, kt, vt,
                 xres, hbuf, wbuf, raw, stage, vstage, qbuf, kbuf, vbuf, scores, acc, kraw, vraw, kturn, vturn, fresh, peak_ref, sum_ref, fade_ref, chunk_max, ahead_ref, outst,
                 wsem, xsem, qsend, qrecv, kvsend, kvrecv, nsend, nrecv, osend, orecv, ksend, krecv, psend, precv, outsem, turnsem,
                 free_sem):
    dp = lax.axis_index("dp")
    me = lax.axis_index("cp")
    chip, core = div(me, 2), rem(me, 2)
    hid = wbuf.shape[1]
    pair = 2 * rows
    new = 8 * rows
    parts = width // TILE
    per_chip = 2 * parts
    tiles = 4 * per_chip
    keys_a = 2 * seg
    keys_b = 2 * seg + new
    coef = math.log2(math.e) * HEAD_DIM ** -0.5
    neg = float("-inf")
    q_tiles = 4 * parts
    p1_tiles = q_tiles + 2
    out_tiles = hid // TILE
    chunk = hid // 4
    turns = 8
    depth = seg // turns

    def device(index):
        return (dp, index)

    partner = flip(me, 1)

    barrier = pltpu.get_barrier_semaphore()
    for rel in range(1, 8):
        pl.semaphore_signal(barrier, inc=1, device_id=device(flip(me, rel)), device_id_type=MESH)

    def remote(src, dst, send, recv, index):
        return pltpu.make_async_remote_copy(
            src_ref=src, dst_ref=dst, send_sem=send, recv_sem=recv, device_id=device(index), device_id_type=MESH)

    my_rows = pl.ds(pl.multiple_of(core * rows, rows), rows)
    other_rows = pl.ds(pl.multiple_of((1 - core) * rows, rows), rows)

    def tile_of(ref, slot, a):
        return ref.at[slot, pl.ds(a * chunk, chunk), :]

    def fetch_kv(ref, n):
        slot = rem(n, WBUFS)
        for a in range(4):
            first = pl.multiple_of((2 * a + core) * HEAD_DIM, HEAD_DIM)
            pltpu.make_async_copy(ref.at[:, pl.ds(first, HEAD_DIM)],
                                  wbuf.at[slot, :, pl.ds(a * HEAD_DIM, HEAD_DIM)], wsem.at[slot, a]).start()

    def fetch_q(n):
        slot = rem(n, WBUFS)
        g, part = div(n - 1, parts), rem(n - 1, parts)
        head = 2 * flip_chip(chip, rem(g + 1, 4)) + core
        first = pl.multiple_of(head * width + part * TILE, TILE)
        for a in range(4):
            pltpu.make_async_copy(wq_in.at[pl.ds(a * chunk, chunk), pl.ds(first, TILE)],
                                  tile_of(wbuf, slot, a), wsem.at[slot, a]).start()

    def fetch_o(m):
        slot = rem(p1_tiles + m, WBUFS)
        first = pl.multiple_of(m * TILE, TILE)
        for a in range(4):
            top = pl.multiple_of((2 * a + core) * width, width)
            pltpu.make_async_copy(wo_in.at[pl.ds(top, width), pl.ds(first, TILE)],
                                  tile_of(wbuf, slot, a), wsem.at[slot, a]).start()

    def wait_tile(n):
        slot = rem(n, WBUFS)
        for a in range(4):
            pltpu.make_async_copy(tile_of(wbuf, slot, a), tile_of(wbuf, slot, a), wsem.at[slot, a]).wait()

    x_local = pltpu.make_async_copy(x_in, hbuf.at[my_rows, :], xsem.at[0])
    x_remote = remote(x_in, hbuf.at[my_rows, :], xsem.at[1], xsem.at[2], partner)
    x_local.start()
    fetch_kv(wk_in, 0)
    with jax.named_scope("barrier"):
        pl.semaphore_wait(barrier, 7)
    x_remote.start()
    fetch_q(1)
    fetch_q(2)

    def kv_copy(p, kind):
        peer = flip(me, ORD[p])
        if kind == 0:
            src, dst = kt.at[peer], kbuf.at[pl.ds(p * seg, seg), :]
        else:
            src, dst = vt.at[peer], vbuf.at[:, pl.ds(p * seg, seg)]
        if p == 0:
            return pltpu.make_async_copy(src, dst, kvrecv.at[kind, 0])
        return remote(src, dst, kvsend.at[kind, p], kvrecv.at[kind, p], peer)

    def kv_send(pair_index):
        for p in (2 * pair_index, 2 * pair_index + 1):
            for kind in range(2):
                kv_copy(p, kind).start()

    def kv_wait(p):
        for kind in range(2):
            if p == 0:
                kv_copy(p, kind).wait()
            else:
                kv_copy(p, kind).wait_recv()

    def turn_in(c):
        where = pl.ds(pl.multiple_of(c * depth, depth), depth)
        slot = rem(c, 2)
        return (pltpu.make_async_copy(k_in.at[where], kraw.at[slot], turnsem.at[0, slot]),
                pltpu.make_async_copy(v_in.at[where], vraw.at[slot], turnsem.at[1, slot]))

    def turn_out(c):
        where = pl.ds(pl.multiple_of(c * depth, depth), depth)
        slot = rem(c, 2)
        return (pltpu.make_async_copy(kturn.at[slot], kt.at[:, where, :], turnsem.at[2, slot]),
                pltpu.make_async_copy(vturn.at[slot], vt.at[:, :, where], turnsem.at[3, slot]))

    def turn(c):
        slot = rem(c, 2)
        acc[pl.ds(0, 8 * depth), :] = kraw[slot].astype(F32).reshape(8 * depth, HEAD_DIM)
        acc[pl.ds(8 * depth, 8 * depth), :] = vraw[slot].astype(F32).reshape(8 * depth, HEAD_DIM)
        for h in range(8):
            kturn[slot, h] = acc[pl.ds(h, depth, stride=8), :].astype(BF16)
            vturn[slot, h] = acc[pl.ds(8 * depth + h, depth, stride=8), :].T.astype(BF16)

    for c in turn_in(0):
        c.start()

    def normalise(first_row):
        def some(i, carry):
            at = pl.multiple_of(first_row + i * 32, 32)
            wide = hbuf[pl.ds(at, 32), :].astype(F32)
            mean_sq = jnp.sum(wide * wide, axis=-1, keepdims=True) * (1.0 / hid)
            hbuf[pl.ds(at, 32), :] = (wide * lax.rsqrt(mean_sq + NORM_EPS) * gain_in[:, :hid]).astype(BF16)
            return carry
        lax.fori_loop(0, rows // 32, some, 0)

    with jax.named_scope("xwait"):
        x_local.wait()
    with jax.named_scope("norm"):
        normalise(core * rows)
    with jax.named_scope("xrwait"):
        x_remote.wait_recv()
    with jax.named_scope("norm"):
        normalise((1 - core) * rows)

    def multiply(n):
        slot = rem(n, WBUFS)
        return jnp.dot(hbuf[...], wbuf[slot], preferred_element_type=F32)

    def rotate(e):
        group, part = div(e + parts - 1, parts), rem(e + parts - 1, parts)
        gain = gain_in[:, pl.ds(pl.multiple_of(hid + jnp.minimum(e, 1) * HEAD_DIM, HEAD_DIM), HEAD_DIM)]
        cos_tab, sin_tab = cos_in[...], sin_in[...]
        done = []
        for h in range(HEADS):
            vals = raw[:, h * HEAD_DIM:(h + 1) * HEAD_DIM].astype(F32)
            mean_sq = jnp.sum(vals * vals, axis=-1, keepdims=True) * (1.0 / HEAD_DIM)
            vals = vals * lax.rsqrt(mean_sq + NORM_EPS) * gain
            done.append((vals * cos_tab + pltpu.roll(vals, HEAD_DIM // 2, 1) * sin_tab).astype(BF16))
        done = jnp.concatenate(done, axis=1)
        where = pl.ds(pl.multiple_of(part * TILE, TILE), TILE)
        stage[group, :, where] = done
        qbuf[0, :, where] = done

    def q_copy(rel, part):
        cols = pl.ds(pl.multiple_of(part * TILE, TILE), TILE)
        return remote(stage.at[rel, :, cols], qbuf.at[rel, :, cols], qsend.at[rel, part], qrecv.at[rel, part],
                      2 * flip_chip(chip, rel) + core)

    def new_copy(rel, kind):
        other = flip_chip(chip, rel)
        here = pl.ds(pl.multiple_of(8 * seg + chip * pair, pair), pair)
        if kind == 0:
            first = pl.multiple_of((parts - 1) * TILE + other * HEAD_DIM, HEAD_DIM)
            src, dst = stage.at[0, :, pl.ds(first, HEAD_DIM)], kbuf.at[here, :]
        else:
            src, dst = vstage.at[other], vbuf.at[:, here]
        return remote(src, dst, nsend.at[kind, rel], nrecv.at[kind, rel], 2 * other + core)

    def new_heads(kind, a):
        if kind == 0:
            return stage.at[0, :, pl.ds((parts - 1) * TILE + a * HEAD_DIM, HEAD_DIM)]
        return raw.at[:, pl.ds(a * HEAD_DIM, HEAD_DIM)]

    def to_partner(kind, a, parity):
        dst = kturn.at[kind, 2 * a + parity, pl.ds(0, rows), :]
        return remote(new_heads(kind, a).at[other_rows, :], dst, ksend.at[kind, a], krecv.at[kind, a], partner)

    wait_tile(0)
    raw[...] = multiply(0).astype(BF16)
    fetch_q(3)

    def project(turning, n, carry):
        @pl.when(n == 2)
        def _():
            for rel in range(1, 4):
                new_copy(rel, 0).start()

        @pl.when((n >= 3) & (n < 3 + 3 * parts))
        def _():
            e = n - 2
            q_copy(div(e + parts - 1, parts), rem(e + parts - 1, parts)).start()

        if turning:
            @pl.when(n < turns)
            def _():
                for c in turn_in(n):
                    c.start()

            with jax.named_scope("turnin"):
                for c in turn_in(n - 1):
                    c.wait()

            @pl.when(n >= 3)
            def _():
                with jax.named_scope("turnout"):
                    for c in turn_out(n - 3):
                        c.wait()
        else:
            @pl.when(n == turns + 1)
            def _():
                for c in (*turn_out(turns - 2), *turn_out(turns - 1)):
                    c.wait()
                for p in range(2):
                    for kind in range(2):
                        kv_copy(p, kind).start()

            @pl.when(n == 3 + 3 * parts)
            def _():
                kv_send(1)

        with jax.named_scope("pwait"):
            wait_tile(n)
        with jax.named_scope("pbody%d" % int(turning)):
            rotate(n - 1)
            if turning:
                turn(n - 1)
            raw[...] = multiply(n).astype(BF16)
        if turning:
            for c in turn_out(n - 1):
                c.start()

        @pl.when(n + WBUFS <= q_tiles)
        def _():
            fetch_q(n + WBUFS)

        @pl.when(n + WBUFS == q_tiles + 1)
        def _():
            fetch_kv(wv_in, q_tiles + 1)

        @pl.when((n + WBUFS >= p1_tiles) & (n + WBUFS < p1_tiles + WBUFS - 1))
        def _():
            fetch_o(n + WBUFS - p1_tiles)

        return carry

    lax.fori_loop(1, turns + 1, functools.partial(project, True), 0)
    lax.fori_loop(turns + 1, p1_tiles, functools.partial(project, False), 0)

    here = pl.ds(pl.multiple_of(8 * seg + chip * pair, pair), pair)
    for a in range(4):
        vstage[a] = raw[:, a * HEAD_DIM:(a + 1) * HEAD_DIM].astype(F32).T.astype(BF16)
    kbuf[here, :] = stage[0, :, pl.ds(pl.multiple_of((parts - 1) * TILE + chip * HEAD_DIM, HEAD_DIM), HEAD_DIM)]
    vbuf[:, here] = vstage[chip]

    def acc_rows(t, h):
        return pl.ds(pl.multiple_of((t * HEADS + h) * HEAD_DIM, HEAD_DIM), HEAD_DIM)

    def init(t, carry):
        peak_ref[t] = jnp.full((1, TILE), neg, F32)
        sum_ref[t] = jnp.zeros((1, TILE), F32)
        for h in range(HEADS):
            acc[acc_rows(t, h), :] = jnp.zeros((HEAD_DIM, rows), F32)
        return carry

    lax.fori_loop(0, tiles, init, 0)
    ahead_ref[...] = (lax.broadcasted_iota(jnp.int32, (SUB, rows), 0)
                      - lax.broadcasted_iota(jnp.int32, (SUB, rows), 1))
    for rel in range(1, 4):
        new_copy(rel, 1).start()

    def place(t):
        rel, rest = div(t, per_chip), rem(t, per_chip)
        return rel, pl.ds(pl.multiple_of(rem(rest, 2) * rows, rows), rows), div(rest, 2)

    def q_tile(t):
        rel, some_rows, part = place(t)
        block = qbuf[rel, some_rows, pl.ds(pl.multiple_of(part * TILE, TILE), TILE)]
        return jnp.concatenate([block[:, h * HEAD_DIM:(h + 1) * HEAD_DIM] for h in range(HEADS)], axis=0)

    probs = wbuf.at[(p1_tiles + WBUFS - 1) % WBUFS]

    def step(pv=None, sm=None, qk=None, end=None):
        if end is not None:
            finish(end)
        if pv is not None:
            t_pv, base_pv, keys_pv = pv
            fade_pv = fade_ref[...]
        if sm is not None:
            t_sm, keys_sm = sm
            old = peak_ref[t_sm]
            top = jnp.maximum(old, jnp.max(chunk_max[...], axis=0, keepdims=True) * coef)
            fade = jnp.exp2(old - top)
            peak_ref[t_sm] = top
        if qk is not None:
            t_qk, base_qk, keys_qk, has_new = qk
            q = q_tile(t_qk)
            first_row = flip_chip(chip, div(t_qk, per_chip)) * pair + rem(t_qk, 2) * rows if has_new else None
        total = None
        values = None
        peaks = None
        most = max(pv[2] if pv else 0, sm[1] if sm else 0, qk[2] if qk else 0)
        for s in range(most // SUB):
            lines = slice(s * SUB, (s + 1) * SUB)
            if pv is not None and s * SUB < keys_pv:
                v_part = vbuf[:, pl.ds(pl.multiple_of(base_pv + s * SUB, SUB), SUB)]
                o_part = jnp.dot(v_part, probs[lines, :], preferred_element_type=F32)
                values = o_part if values is None else values + o_part
            if sm is not None and s * SUB < keys_sm:
                w = jnp.exp2(scores[lines, :] * coef - top)
                part = jnp.sum(w.reshape(SUB // 8, 8, TILE), axis=0)
                total = part if total is None else total + part
                probs[lines, :] = w.astype(BF16)
            if qk is not None and s * SUB < keys_qk:
                k_part = kbuf[pl.ds(pl.multiple_of(base_qk + s * SUB, SUB), SUB), :]
                sc = lax.dot_general(k_part, q, (((1,), (1,)), ((), ())), preferred_element_type=F32)
                if has_new and s * SUB >= keys_a:
                    seen = ahead_ref[...] <= first_row - (s * SUB - keys_a)
                    sc = jnp.concatenate(
                        [jnp.where(seen, sc[:, h * rows:(h + 1) * rows], neg) for h in range(HEADS)], axis=1)
                scores[lines, :] = sc
                part = jnp.max(sc.reshape(SUB // 8, 8, TILE), axis=0)
                peaks = part if peaks is None else jnp.maximum(peaks, part)
        if qk is not None:
            chunk_max[...] = peaks
        if sm is not None:
            sum_ref[t_sm] = sum_ref[t_sm] * fade + jnp.sum(total, axis=0, keepdims=True)
            fade_ref[...] = fade
        if pv is not None:
            for h in range(HEADS):
                cols = slice(h * rows, (h + 1) * rows)
                acc[acc_rows(t_pv, h), :] = acc[acc_rows(t_pv, h), :] * fade_pv[:, cols] + values[:, cols]

    def finish(t):
        sums = sum_ref[t]
        rel, some_rows, part = place(t)
        done = jnp.concatenate(
            [(acc[acc_rows(t, h), :] / sums[:, h * rows:(h + 1) * rows]).T.astype(BF16) for h in range(HEADS)], axis=1)
        stage[rel, some_rows, pl.ds(pl.multiple_of(part * TILE, TILE), TILE)] = done
        hbuf[some_rows, pl.ds(pl.multiple_of(chip * width + part * TILE, TILE), TILE)] = done

    steps_a = 3 * tiles

    def item_a(i):
        return rem(i, tiles), div(i, tiles) * keys_a, keys_a

    with jax.named_scope("kv01wait"):
        kv_wait(0)
        kv_wait(1)
    for kind in range(2):
        for a in range(4):
            kturn[kind, 2 * a + core, :rows] = new_heads(kind, a)[my_rows, :]
            to_partner(kind, a, core).start()
    step(qk=(*item_a(0), False))
    step(sm=(0, keys_a), qk=(*item_a(1), False))

    def body_a(i, carry):
        nxt = i + 1

        @pl.when((nxt >= per_chip) & (nxt < tiles) & (rem(nxt, 2) == 0))
        def _():
            with jax.named_scope("qwait"):
                q_copy(div(nxt, per_chip), div(rem(nxt, per_chip), 2)).wait_recv()

        @pl.when(nxt == 2 * tiles // 3)
        def _():
            kv_send(2)

        @pl.when(nxt == 4 * tiles // 3)
        def _():
            kv_send(3)

        for v in (1, 2):
            @pl.when(nxt == v * tiles)
            def _():
                with jax.named_scope("kvwait"):
                    kv_wait(2 * v)
                    kv_wait(2 * v + 1)
        with jax.named_scope("abody"):
            step(pv=item_a(i - 1), sm=(rem(i, tiles), keys_a), qk=(*item_a(nxt), False))
        return carry

    lax.fori_loop(1, steps_a - 1, body_a, 0)

    with jax.named_scope("kv67wait"):
        kv_wait(6)
        kv_wait(7)
    for rel in range(1, 4):
        new_copy(rel, 0).wait_recv()
        new_copy(rel, 1).wait_recv()
        new_copy(rel, 0).wait_send()
        for part in range(parts):
            q_copy(rel, part).wait_send()
    for a in range(4):
        to_partner(0, a, core).wait_send()

    def tile_b(i):
        return (3 - div(i, per_chip)) * per_chip + rem(i, per_chip)

    def o_copy(rel, part):
        cols = pl.ds(pl.multiple_of(part * TILE, TILE), TILE)
        there = pl.ds(pl.multiple_of(chip * width + part * TILE, TILE), TILE)
        return remote(stage.at[rel, :, cols], hbuf.at[:, there], osend.at[rel, part], orecv.at[rel, part],
                      2 * flip_chip(chip, rel) + core)

    def o_arrival(rel, part):
        there = pl.ds(pl.multiple_of(flip_chip(chip, rel) * width + part * TILE, TILE), TILE)
        return remote(hbuf.at[:, there], hbuf.at[:, there], osend.at[rel, part], orecv.at[rel, part],
                      2 * flip_chip(chip, rel) + core)

    base_b = 3 * keys_a

    def item_b(i):
        return tile_b(i), base_b, keys_b

    step(pv=item_a(steps_a - 2), sm=((steps_a - 1) % tiles, keys_a), qk=(*item_b(0), True))
    step(pv=item_a(steps_a - 1), sm=(tile_b(0), keys_b), qk=(*item_b(1), True))
    step(pv=item_b(0), sm=(tile_b(1), keys_b), qk=(*item_b(2), True))

    def body_b(i, carry):
        @pl.when((i >= 4) & (rem(i, 2) == 0) & (i <= 3 * per_chip + 2))
        def _():
            done = i - 4
            o_copy(3 - div(done, per_chip), div(rem(done, per_chip), 2)).start()

        with jax.named_scope("bbody"):
            step(pv=item_b(i - 1), sm=(tile_b(i), keys_b), qk=(*item_b(i + 1), True), end=tile_b(i - 2))
        return carry

    lax.fori_loop(2, tiles - 1, body_b, 0)
    step(pv=item_b(tiles - 2), sm=(tile_b(tiles - 1), keys_b), end=tile_b(tiles - 3))
    step(pv=item_b(tiles - 1), end=tile_b(tiles - 2))
    finish(tile_b(tiles - 1))
    fetch_o(WBUFS - 1)

    pl.semaphore_signal(free_sem, inc=1, device_id=device(partner), device_id_type=MESH)
    with jax.named_scope("owait"):
        for rel in range(1, 4):
            for part in range(parts):
                o_arrival(rel, part).wait_recv()
        pl.semaphore_wait(free_sem, 1)

    for kind in range(2):
        for a in range(4):
            to_partner(kind, a, 1 - core).wait_recv()
        for h in range(8):
            acc[pl.ds(kind * 8 * rows + h, rows, stride=8), :] = kturn[kind, h, :rows].astype(F32)
        flat = acc[pl.ds(kind * 8 * rows, 8 * rows), :].astype(BF16)
        fresh[kind] = flat.reshape(rows, 8, HEAD_DIM)
    new_out = (pltpu.make_async_copy(fresh.at[0], k_out, turnsem.at[0, 0]),
               pltpu.make_async_copy(fresh.at[1], v_out, turnsem.at[0, 1]))
    for c in new_out:
        c.start()

    sent, got, own = 0, out_tiles * rows, 2 * out_tiles * rows

    def lines(first, m):
        return pl.ds(pl.multiple_of(first + m * rows, rows), rows)

    def p_copy(m):
        return remote(scores.at[lines(sent, m), :], scores.at[lines(got, m), :], psend.at[m], precv.at[m], partner)

    def out_copy(m):
        cols = pl.ds(pl.multiple_of(m * TILE, TILE), TILE)
        return pltpu.make_async_copy(outst.at[rem(m, 2)], out.at[:, cols], outsem.at[m])

    def x_copy(m):
        cols = pl.ds(pl.multiple_of(m * TILE, TILE), TILE)
        return pltpu.make_async_copy(x_in.at[:, cols], xres.at[rem(m, 2)], xsem.at[3 + rem(m, 2)])

    def combine(m):
        if isinstance(m, int):
            out_copy(m - 2).wait()
        else:
            @pl.when(m >= 2)
            def _():
                out_copy(m - 2).wait()
        with jax.named_scope("cwait"):
            p_copy(m).wait_recv()
            x_copy(m).wait()
        both = scores[lines(own, m), :] + scores[lines(got, m), :]
        outst[rem(m, 2)] = (xres[rem(m, 2)].astype(F32) + both).astype(BF16)
        out_copy(m).start()

    def output(m, carry):
        @pl.when(m >= 1)
        def _():
            p_copy(m - 1).start()

        @pl.when(m >= 2)
        def _():
            combine(m - 2)

        x_copy(m).start()
        with jax.named_scope("otilewait"):
            wait_tile(p1_tiles + m)
        both = multiply(p1_tiles + m)
        scores[lines(own, m), :] = jnp.where(core == 0, both[:rows], both[rows:])
        scores[lines(sent, m), :] = jnp.where(core == 0, both[rows:], both[:rows])

        @pl.when(m + WBUFS < out_tiles)
        def _():
            fetch_o(m + WBUFS)

        return carry

    lax.fori_loop(0, out_tiles, output, 0)
    p_copy(out_tiles - 1).start()
    combine(out_tiles - 2)
    combine(out_tiles - 1)

    def drain(m, carry):
        p_copy(m).wait_send()
        return carry

    with jax.named_scope("drain"):
        lax.fori_loop(0, out_tiles, drain, 0)
    out_copy(out_tiles - 2).wait()
    out_copy(out_tiles - 1).wait()
    x_remote.wait_send()
    for p in range(1, 8):
        for kind in range(2):
            kv_copy(p, kind).wait_send()
    for rel in range(1, 4):
        new_copy(rel, 1).wait_send()
        for part in range(parts):
            o_copy(rel, part).wait_send()
    for a in range(4):
        to_partner(1, a, core).wait_send()
    for c in new_out:
        c.wait()


def block(x, k_cache, v_cache, gains, cos_tab, sin_tab, w_q, w_k, w_v, w_o):
    rows, hid = x.shape
    seg = k_cache.shape[0]
    width = w_q.shape[1] // 8
    pair, new = 2 * rows, 8 * rows
    parts = width // TILE
    tiles = 8 * parts
    out_tiles = hid // TILE
    keys_b = 2 * seg + new
    flops = 4 * (8 * seg + new) * 8 * rows * width + 8 * rows * hid * width * 2
    hbm = pl.BlockSpec(memory_space=pl.ANY)
    vmem = pl.BlockSpec(memory_space=pltpu.VMEM)
    dma = pltpu.SemaphoreType.DMA
    return pl.pallas_call(
        functools.partial(block_kernel, rows, seg, width),
        out_shape=(
            jax.ShapeDtypeStruct((rows, hid), BF16),
            jax.ShapeDtypeStruct((rows, 8, HEAD_DIM), BF16),
            jax.ShapeDtypeStruct((rows, 8, HEAD_DIM), BF16),
            jax.ShapeDtypeStruct((8, seg, HEAD_DIM), BF16),
            jax.ShapeDtypeStruct((8, HEAD_DIM, seg), BF16),
        ),
        in_specs=[hbm, hbm, hbm, vmem, vmem, vmem, hbm, hbm, hbm, hbm],
        out_specs=(hbm,) * 5,
        scratch_shapes=[
            pltpu.VMEM((2, rows, TILE), BF16),
            pltpu.VMEM((pair, hid), BF16),
            pltpu.VMEM((WBUFS, hid, TILE), BF16),
            pltpu.VMEM((pair, TILE), BF16),
            pltpu.VMEM((5, pair, width), BF16),
            pltpu.VMEM((4, HEAD_DIM, pair), BF16),
            pltpu.VMEM((4, pair, width), BF16),
            pltpu.VMEM((8 * seg + new, HEAD_DIM), BF16),
            pltpu.VMEM((HEAD_DIM, 8 * seg + new), BF16),
            pltpu.VMEM((max(keys_b, 3 * out_tiles * rows), TILE), F32),
            pltpu.VMEM((tiles * HEADS * HEAD_DIM, rows), F32),
            pltpu.VMEM((2, seg // 8, 8, HEAD_DIM), BF16),
            pltpu.VMEM((2, seg // 8, 8, HEAD_DIM), BF16),
            pltpu.VMEM((2, 8, seg // 8, HEAD_DIM), BF16),
            pltpu.VMEM((2, 8, HEAD_DIM, seg // 8), BF16),
            pltpu.VMEM((2, rows, 8, HEAD_DIM), BF16),
            pltpu.VMEM((tiles, 1, TILE), F32),
            pltpu.VMEM((tiles, 1, TILE), F32),
            pltpu.VMEM((1, TILE), F32),
            pltpu.VMEM((8, TILE), F32),
            pltpu.VMEM((SUB, rows), jnp.int32),
            pltpu.VMEM((2, rows, TILE), BF16),
            dma((WBUFS, 4)),
            dma((5,)),
            dma((4, parts)), dma((4, parts)),
            dma((2, 8)), dma((2, 8)),
            dma((2, 4)), dma((2, 4)),
            dma((4, parts)), dma((4, parts)),
            dma((2, 4)), dma((2, 4)),
            dma((out_tiles,)), dma((out_tiles,)),
            dma((out_tiles,)),
            dma((4, 2)),
            pltpu.SemaphoreType.REGULAR,
        ],
        compiler_params=pltpu.CompilerParams(
            collective_id=0, has_side_effects=True, vmem_limit_bytes=67043328),
        cost_estimate=pl.CostEstimate(flops=flops, bytes_accessed=200 * 1024 * 1024, transcendentals=flops // 512),
        name="block",
    )(x, k_cache, v_cache, gains, cos_tab, sin_tab, w_q, w_k, w_v, w_o)


def solution(mesh):
    cp_size = mesh.shape['cp']
    row_spec = P(('dp', 'cp'), None)
    cache_spec = P(('dp', 'cp'), None, None)
    whole = P()

    def device_step(x_rows, k_cache, v_cache, ln_gain, w_q, w_k, w_v, w_o, q_gain, k_gain):
        rows = x_rows.shape[0]
        prefix_len = k_cache.shape[0] * cp_size
        chip = lax.axis_index('cp') // 2
        positions = (prefix_len + chip * 2 * rows + jnp.arange(2 * rows)).astype(F32)
        lane = jnp.arange(HEAD_DIM)
        half = HEAD_DIM // 2
        inv_freq = ROPE_THETA ** (-(lane % half).astype(F32) * (2.0 / HEAD_DIM))
        angles = positions[:, None] * inv_freq[None, :]
        cos_tab = jnp.cos(angles)
        sin_tab = jnp.sin(angles) * jnp.where(lane < half, -1.0, 1.0)[None, :]
        gains = jnp.concatenate([ln_gain, k_gain, q_gain]).astype(F32)[None, :]
        out, k_new, v_new, _, _ = block(
            x_rows, k_cache, v_cache, gains, cos_tab, sin_tab, w_q, w_k, w_v, w_o)
        return out, k_new, v_new

    return jax.shard_map(device_step, mesh=mesh, in_specs=(row_spec, cache_spec, cache_spec, whole, whole, whole, whole, whole, whole, whole), out_specs=(row_spec, cache_spec, cache_spec), check_vma=False)
```

```python
import functools
import math

import jax
import jax.numpy as jnp
from jax import lax
from jax.experimental import pallas as pl
from jax.experimental.pallas import tpu as pltpu
from jax.sharding import PartitionSpec as P

HEAD_DIM = 128
ROPE_THETA = 1.0e6
NORM_EPS = 1.0e-6
MESH = pl.DeviceIdType.MESH
F32 = jnp.float32
BF16 = jnp.bfloat16

ORD = (0, 1, 2, 4, 3, 5, 6, 7)
SUB = 256
TILE = 512
HEADS = TILE // HEAD_DIM
WBUFS = 3
RAWS = 3
CHIPS = 4


def div(a, b):
    return a // b if isinstance(a, int) else lax.div(a, jnp.int32(b))


def rem(a, b):
    return a % b if isinstance(a, int) else lax.rem(a, jnp.int32(b))


def flip(me, rel):
    out = 0
    for bit in (1, 2, 4):
        mine = rem(div(me, bit), 2)
        out = out + bit * ((1 - mine) if rel & bit else mine)
    return out


def flip_chip(chip, rel):
    return rem(rem(chip, 2) + rem(rel, 2), 2) + 2 * rem(div(chip, 2) + div(rel, 2), 2)


def block_kernel(rows, seg, width,
                 x_in, k_in, v_in, ln_in, kg_in, qg_in, cos_in, sin_in, wq_in, wk_in, wv_in, wo_in,
                 out, k_out, v_out, kt, vt,
                 xres, gains, hbuf, wbuf, raw, stage, vstage, qbuf, kbuf, vbuf, scores, acc, kraw, vraw, kturn, vturn, peak_ref, sum_ref, fade_ref, chunk_max, ahead_ref, outst,
                 wsem, xsem, qsend, qrecv, kvsend, kvrecv, nsend, nrecv, osend, orecv, ksend, krecv, psend, precv, outsem, turnsem,
                 free_sem):
    dp = lax.axis_index("dp")
    me = lax.axis_index("cp")
    chip, core = div(me, 2), rem(me, 2)
    hid = wbuf.shape[1]
    pair = 2 * rows
    new = 8 * rows
    parts = width // TILE
    per_chip = 2 * parts
    tiles = 4 * per_chip
    keys_a = 2 * seg
    keys_b = 2 * seg + new
    coef = math.log2(math.e) * HEAD_DIM ** -0.5
    neg = float("-inf")
    q_tiles = 4 * parts
    p1_tiles = q_tiles + 2
    out_tiles = hid // TILE
    cached = 8 * seg
    others = range(1, CHIPS)
    chunk = hid // 4
    turns = 8
    cleared = acc.shape[0] // (p1_tiles - turns)
    depth = seg // turns

    def device(index):
        return (dp, index)

    partner = flip(me, 1)

    my_rows = pl.ds(pl.multiple_of(core * rows, rows), rows)
    other_rows = pl.ds(pl.multiple_of((1 - core) * rows, rows), rows)
    x_local = pltpu.make_async_copy(x_in, hbuf.at[my_rows, :], xsem.at[0])
    x_local.start()

    barrier = pltpu.get_barrier_semaphore()
    for rel in range(1, 8):
        pl.semaphore_signal(barrier, inc=1, device_id=device(flip(me, rel)), device_id_type=MESH)

    def remote(src, dst, send, recv, index):
        return pltpu.make_async_remote_copy(
            src_ref=src, dst_ref=dst, send_sem=send, recv_sem=recv, device_id=device(index), device_id_type=MESH)

    def tile_of(ref, slot, a):
        return ref.at[slot, pl.ds(a * chunk, chunk), :]

    def fetch_kv(ref, n):
        slot = rem(n, WBUFS)
        for a in range(CHIPS):
            first = pl.multiple_of((2 * a + core) * HEAD_DIM, HEAD_DIM)
            pltpu.make_async_copy(ref.at[:, pl.ds(first, HEAD_DIM)],
                                  wbuf.at[slot, :, pl.ds(a * HEAD_DIM, HEAD_DIM)], wsem.at[slot, a]).start()

    def fetch_q(n):
        slot = rem(n, WBUFS)
        g, part = div(n - 1, parts), rem(n - 1, parts)
        head = 2 * flip_chip(chip, rem(g + 1, 4)) + core
        first = pl.multiple_of(head * width + part * TILE, TILE)
        for a in range(CHIPS):
            pltpu.make_async_copy(wq_in.at[pl.ds(a * chunk, chunk), pl.ds(first, TILE)],
                                  tile_of(wbuf, slot, a), wsem.at[slot, a]).start()

    def fetch_o(m):
        slot = rem(p1_tiles + m, WBUFS)
        first = pl.multiple_of(m * TILE, TILE)
        for a in range(CHIPS):
            top = pl.multiple_of((2 * a + core) * width, width)
            pltpu.make_async_copy(wo_in.at[pl.ds(top, width), pl.ds(first, TILE)],
                                  tile_of(wbuf, slot, a), wsem.at[slot, a]).start()

    def wait_tile(n):
        slot = rem(n, WBUFS)
        for a in range(CHIPS):
            pltpu.make_async_copy(tile_of(wbuf, slot, a), tile_of(wbuf, slot, a), wsem.at[slot, a]).wait()

    def turn_in(c):
        where = pl.ds(pl.multiple_of(c * depth, depth), depth)
        slot = rem(c, RAWS)
        return (pltpu.make_async_copy(k_in.at[where], kraw.at[slot], turnsem.at[0, slot]),
                pltpu.make_async_copy(v_in.at[where], vraw.at[slot], turnsem.at[1, slot]))

    def turn_out(c):
        where = pl.ds(pl.multiple_of(c * depth, depth), depth)
        slot = rem(c, 2)
        return (pltpu.make_async_copy(kturn.at[slot], kt.at[:, where, :], turnsem.at[2, slot]),
                pltpu.make_async_copy(vturn.at[slot], vt.at[:, :, where], turnsem.at[3, slot]))

    def turn(c):
        slot, here = rem(c, 2), rem(c, RAWS)
        acc[pl.ds(0, 8 * depth), :] = kraw[here].astype(F32).reshape(8 * depth, HEAD_DIM)
        acc[pl.ds(8 * depth, 8 * depth), :] = vraw[here].astype(F32).reshape(8 * depth, HEAD_DIM)
        for h in range(8):
            kturn[slot, h] = acc[pl.ds(h, depth, stride=8), :].astype(BF16)
            vturn[slot, h] = acc[pl.ds(8 * depth + h, depth, stride=8), :].T.astype(BF16)

    x_remote = remote(x_in, hbuf.at[my_rows, :], xsem.at[1], xsem.at[2], partner)
    x_local.wait()
    for c in turn_in(0):
        c.start()
    fetch_kv(wk_in, 0)
    for piece in range(1, RAWS):
        for c in turn_in(piece):
            c.start()
    pl.semaphore_wait(barrier, 7)
    x_remote.start()
    fetch_q(1)
    fetch_q(2)

    def kv_copy(p, kind):
        peer = flip(me, ORD[p])
        if kind == 0:
            src, dst = kt.at[peer], kbuf.at[pl.ds(p * seg, seg), :]
        else:
            src, dst = vt.at[peer], vbuf.at[:, pl.ds(p * seg, seg)]
        if p == 0:
            return pltpu.make_async_copy(src, dst, kvrecv.at[kind, 0])
        return remote(src, dst, kvsend.at[kind, p], kvrecv.at[kind, p], peer)

    def kv_send(pair_index):
        for p in (2 * pair_index, 2 * pair_index + 1):
            for kind in range(2):
                kv_copy(p, kind).start()

    def kv_wait(p):
        for kind in range(2):
            if p == 0:
                kv_copy(p, kind).wait()
            else:
                kv_copy(p, kind).wait_recv()

    def normalise(first_row):
        def some(i, carry):
            at = pl.multiple_of(first_row + i * 32, 32)
            wide = hbuf[pl.ds(at, 32), :].astype(F32)
            mean_sq = jnp.sum(wide * wide, axis=-1, keepdims=True) * (1.0 / hid)
            hbuf[pl.ds(at, 32), :] = (wide * lax.rsqrt(mean_sq + NORM_EPS) * gains[:, :hid]).astype(BF16)
            return carry
        lax.fori_loop(0, rows // 32, some, 0)

    for r in range(hid // HEAD_DIM):
        gains[:, r * HEAD_DIM:(r + 1) * HEAD_DIM] = ln_in[r:r + 1, :].astype(F32)
    gains[:, hid:hid + HEAD_DIM] = kg_in[...].astype(F32)
    gains[:, hid + HEAD_DIM:] = qg_in[...].astype(F32)
    normalise(core * rows)
    for c in turn_in(0):
        c.wait()
    turn(0)
    for c in (*turn_out(0), *turn_in(RAWS)):
        c.start()
    x_remote.wait_recv()
    normalise((1 - core) * rows)

    def multiply(n):
        slot = rem(n, WBUFS)
        return jnp.dot(hbuf[...], wbuf[slot], preferred_element_type=F32)

    def rotate(e):
        group, part = div(e + parts - 1, parts), rem(e + parts - 1, parts)
        gain = gains[:, pl.ds(pl.multiple_of(hid + jnp.minimum(e, 1) * HEAD_DIM, HEAD_DIM), HEAD_DIM)]
        cos_tab, sin_tab = cos_in[...], sin_in[...]
        done = []
        for h in range(HEADS):
            vals = raw[:, h * HEAD_DIM:(h + 1) * HEAD_DIM].astype(F32)
            mean_sq = jnp.sum(vals * vals, axis=-1, keepdims=True) * (1.0 / HEAD_DIM)
            vals = vals * lax.rsqrt(mean_sq + NORM_EPS) * gain
            done.append((vals * cos_tab + pltpu.roll(vals, HEAD_DIM // 2, 1) * sin_tab).astype(BF16))
        done = jnp.concatenate(done, axis=1)
        where = pl.ds(pl.multiple_of(part * TILE, TILE), TILE)
        stage[group, :, where] = done
        qbuf[0, :, where] = done

    def q_copy(rel, part):
        cols = pl.ds(pl.multiple_of(part * TILE, TILE), TILE)
        return remote(stage.at[rel, :, cols], qbuf.at[rel, :, cols], qsend.at[rel, part], qrecv.at[rel, part],
                      2 * flip_chip(chip, rel) + core)

    def new_copy(rel, kind):
        other = flip_chip(chip, rel)
        here = pl.ds(pl.multiple_of(cached + chip * pair, pair), pair)
        if kind == 0:
            first = pl.multiple_of((parts - 1) * TILE + other * HEAD_DIM, HEAD_DIM)
            src, dst = stage.at[0, :, pl.ds(first, HEAD_DIM)], kbuf.at[here, :]
        else:
            src, dst = vstage.at[other], vbuf.at[:, here]
        return remote(src, dst, nsend.at[kind, rel], nrecv.at[kind, rel], 2 * other + core)

    def new_heads(kind, a):
        if kind == 0:
            return stage.at[0, :, pl.ds((parts - 1) * TILE + a * HEAD_DIM, HEAD_DIM)]
        return raw.at[:, pl.ds(a * HEAD_DIM, HEAD_DIM)]

    def to_partner(kind, a, parity):
        dst = kturn.at[kind, 2 * a + parity, pl.ds(0, rows), :]
        return remote(new_heads(kind, a).at[other_rows, :], dst, ksend.at[kind, a], krecv.at[kind, a], partner)

    wait_tile(0)
    raw[...] = multiply(0).astype(BF16)
    fetch_q(3)

    def project(turning, n, carry):
        @pl.when(n == 2)
        def _():
            for rel in others:
                new_copy(rel, 0).start()

        @pl.when((n >= 3) & (n < 3 + 3 * parts))
        def _():
            e = n - 2
            q_copy(div(e + parts - 1, parts), rem(e + parts - 1, parts)).start()

        if turning:
            for c in turn_in(n):
                c.wait()

            @pl.when(n >= 2)
            def _():
                for c in turn_out(n - 2):
                    c.wait()
        else:
            @pl.when(n == turns)
            def _():
                for c in (*turn_out(turns - 2), *turn_out(turns - 1)):
                    c.wait()
                for p in range(2):
                    for kind in range(2):
                        kv_copy(p, kind).start()

            @pl.when(n == 3 + 3 * parts)
            def _():
                kv_send(1)

        wait_tile(n)
        rotate(n - 1)
        if turning:
            turn(n)
        else:
            acc[pl.ds(pl.multiple_of((n - turns) * cleared, cleared), cleared), :] = jnp.zeros((cleared, rows), F32)
        raw[...] = multiply(n).astype(BF16)
        if turning:
            for c in turn_out(n):
                c.start()

            @pl.when(n + RAWS < turns)
            def _():
                for c in turn_in(n + RAWS):
                    c.start()

        @pl.when(n + WBUFS <= q_tiles)
        def _():
            fetch_q(n + WBUFS)

        @pl.when(n + WBUFS == q_tiles + 1)
        def _():
            fetch_kv(wv_in, q_tiles + 1)

        @pl.when((n + WBUFS >= p1_tiles) & (n + WBUFS < p1_tiles + WBUFS - 1))
        def _():
            fetch_o(n + WBUFS - p1_tiles)

        return carry

    lax.fori_loop(1, turns, functools.partial(project, True), 0)
    lax.fori_loop(turns, p1_tiles, functools.partial(project, False), 0)

    here = pl.ds(pl.multiple_of(cached + chip * pair, pair), pair)
    for a in range(CHIPS):
        vstage[a] = raw[:, a * HEAD_DIM:(a + 1) * HEAD_DIM].astype(F32).T.astype(BF16)
    kbuf[here, :] = stage[0, :, pl.ds(pl.multiple_of((parts - 1) * TILE + chip * HEAD_DIM, HEAD_DIM), HEAD_DIM)]
    vbuf[:, here] = vstage[chip]

    def acc_rows(t, h):
        return pl.ds(pl.multiple_of((t * HEADS + h) * HEAD_DIM, HEAD_DIM), HEAD_DIM)

    def init(t, carry):
        peak_ref[t] = jnp.full((1, TILE), neg, F32)
        sum_ref[t] = jnp.zeros((1, TILE), F32)
        return carry

    lax.fori_loop(0, tiles, init, 0)
    ahead_ref[...] = (lax.broadcasted_iota(jnp.int32, (SUB, rows), 0)
                      - lax.broadcasted_iota(jnp.int32, (SUB, rows), 1))
    for rel in others:
        new_copy(rel, 1).start()

    def q_tile(rel, half, part):
        some_rows = pl.ds(pl.multiple_of(half * rows, rows), rows)
        block = qbuf[rel, some_rows, pl.ds(pl.multiple_of(part * TILE, TILE), TILE)]
        return jnp.concatenate([block[:, h * HEAD_DIM:(h + 1) * HEAD_DIM] for h in range(HEADS)], axis=0)

    probs = wbuf.at[(p1_tiles + WBUFS - 1) % WBUFS]

    def step(pv=None, sm=None, qk=None, end=None):
        if end is not None:
            finish(*end)
        if pv is not None:
            t_pv, base_pv, keys_pv = pv
            fade_pv = fade_ref[...]
        if sm is not None:
            t_sm, keys_sm = sm
            old = peak_ref[t_sm]
            top = jnp.maximum(old, jnp.max(chunk_max[...], axis=0, keepdims=True) * coef)
            fade = jnp.exp2(old - top)
            peak_ref[t_sm] = top
        if qk is not None:
            rel_qk, half_qk, part_qk, base_qk, keys_qk, has_new = qk
            q = q_tile(rel_qk, half_qk, part_qk)
            first_row = flip_chip(chip, rel_qk) * pair + half_qk * rows if has_new else None
        total = None
        values = None
        peaks = None
        most = max(pv[2] if pv else 0, sm[1] if sm else 0, qk[4] if qk else 0)
        for s in range(most // SUB):
            lines = slice(s * SUB, (s + 1) * SUB)
            if pv is not None and s * SUB < keys_pv:
                v_part = vbuf[:, pl.ds(pl.multiple_of(base_pv + s * SUB, SUB), SUB)]
                o_part = jnp.dot(v_part, probs[lines, :], preferred_element_type=F32)
                values = o_part if values is None else values + o_part
            if sm is not None and s * SUB < keys_sm:
                w = jnp.exp2(scores[lines, :] * coef - top)
                part = jnp.sum(w.reshape(SUB // 8, 8, TILE), axis=0)
                total = part if total is None else total + part
                probs[lines, :] = w.astype(BF16)
            if qk is not None and s * SUB < keys_qk:
                k_part = kbuf[pl.ds(pl.multiple_of(base_qk + s * SUB, SUB), SUB), :]
                sc = lax.dot_general(k_part, q, (((1,), (1,)), ((), ())), preferred_element_type=F32)
                if has_new and s * SUB >= keys_a:
                    seen = ahead_ref[...] <= first_row - (s * SUB - keys_a)
                    sc = jnp.concatenate(
                        [jnp.where(seen, sc[:, h * rows:(h + 1) * rows], neg) for h in range(HEADS)], axis=1)
                scores[lines, :] = sc
                part = jnp.max(sc.reshape(SUB // 8, 8, TILE), axis=0)
                peaks = part if peaks is None else jnp.maximum(peaks, part)
        if qk is not None:
            chunk_max[...] = peaks
        if sm is not None:
            sum_ref[t_sm] = sum_ref[t_sm] * fade + jnp.sum(total, axis=0, keepdims=True)
            fade_ref[...] = fade
        if pv is not None:
            for h in range(HEADS):
                cols = slice(h * rows, (h + 1) * rows)
                acc[acc_rows(t_pv, h), :] = acc[acc_rows(t_pv, h), :] * fade_pv[:, cols] + values[:, cols]

    def finish(rel, half, part):
        t = rel * per_chip + 2 * part + half
        some_rows = pl.ds(pl.multiple_of(half * rows, rows), rows)
        sums = sum_ref[t]
        done = jnp.concatenate(
            [(acc[acc_rows(t, h), :] / sums[:, h * rows:(h + 1) * rows]).T.astype(BF16) for h in range(HEADS)], axis=1)
        stage[rel, some_rows, pl.ds(pl.multiple_of(part * TILE, TILE), TILE)] = done
        hbuf[some_rows, pl.ds(pl.multiple_of(chip * width + part * TILE, TILE), TILE)] = done

    kv_wait(0)
    kv_wait(1)
    for kind in range(2):
        for a in range(CHIPS):
            kturn[kind, 2 * a + core, :rows] = new_heads(kind, a)[my_rows, :]
            to_partner(kind, a, core).start()

    def halves(u):
        part = div(u, 2)
        return u - 2 * part, part

    step(qk=(0, 0, 0, 0, keys_a, False))
    step(sm=(0, keys_a), qk=(0, *halves(1), 0, keys_a, False))

    def below(u, limit):
        return jnp.minimum(jnp.maximum(limit - u, 0), 1)

    def group_a(g, carry):
        visit = div(g, CHIPS)
        rel = g - CHIPS * visit
        for r in others:
            @pl.when(g == r)
            def _():
                for part in range(parts):
                    q_copy(r, part).wait_recv()

        for v in (1, 2):
            @pl.when(g == CHIPS * v)
            def _():
                kv_wait(2 * v)
                kv_wait(2 * v + 1)

        @pl.when(g == 3)
        def _():
            kv_send(2)

        @pl.when(g == 6)
        def _():
            kv_send(3)

        def body_a(u, carry):
            t = rel * per_chip + u
            wrap = below(t, 2)
            step(pv=(t - 2 + tiles * wrap, (visit - wrap) * keys_a, keys_a),
                 sm=(t - 1 + tiles * below(t, 1), keys_a),
                 qk=(rel, *halves(u), visit * keys_a, keys_a, False))
            return carry

        lax.fori_loop(2 * below(g, 1), per_chip, body_a, carry)
        return carry

    lax.fori_loop(0, 3 * CHIPS, group_a, 0)

    kv_wait(6)
    kv_wait(7)
    for rel in others:
        new_copy(rel, 0).wait_recv()
        new_copy(rel, 1).wait_recv()
        new_copy(rel, 0).wait_send()
        for part in range(parts):
            q_copy(rel, part).wait_send()
    for a in range(CHIPS):
        to_partner(0, a, core).wait_send()

    def o_copy(rel, part):
        cols = pl.ds(pl.multiple_of(part * TILE, TILE), TILE)
        there = pl.ds(pl.multiple_of(chip * width + part * TILE, TILE), TILE)
        return remote(stage.at[rel, :, cols], hbuf.at[:, there], osend.at[rel, part], orecv.at[rel, part],
                      2 * flip_chip(chip, rel) + core)

    def o_arrival(rel, part):
        there = pl.ds(pl.multiple_of(flip_chip(chip, rel) * width + part * TILE, TILE), TILE)
        return remote(hbuf.at[:, there], hbuf.at[:, there], osend.at[rel, part], orecv.at[rel, part],
                      2 * flip_chip(chip, rel) + core)

    base_b = 3 * keys_a
    wide = (base_b, keys_b)

    step(pv=(tiles - 2, 2 * keys_a, keys_a), sm=(tiles - 1, keys_a), qk=(3, 0, 0, *wide, True))
    step(pv=(tiles - 1, 2 * keys_a, keys_a), sm=(3 * per_chip, keys_b), qk=(3, *halves(1), *wide, True))
    step(pv=(3 * per_chip, *wide), sm=(3 * per_chip + 1, keys_b), qk=(3, *halves(2), *wide, True))

    def group_b(g, carry):
        rel = 3 - g

        def body_b(u, carry):
            n = g * per_chip + u

            @pl.when((rem(n, 2) == 1) & (n >= 5) & (n < 5 + 3 * per_chip))
            def _():
                done = n - 5
                o_copy(3 - div(done, per_chip), div(rem(done, per_chip), 2)).start()

            t = rel * per_chip + u
            early = below(u, 3)
            step(pv=(t - 2 + 2 * per_chip * below(u, 2), *wide),
                 sm=(t - 1 + 2 * per_chip * below(u, 1), keys_b),
                 qk=(rel, *halves(u), *wide, True),
                 end=(rel + early, *halves(u - 3 + per_chip * early)))
            return carry

        lax.fori_loop(3 * below(g, 1), per_chip, body_b, carry)
        return carry

    lax.fori_loop(0, CHIPS, group_b, 0)
    last = per_chip - 1
    step(pv=(last - 1, *wide), sm=(last, keys_b), end=(0, *halves(last - 2)))
    step(pv=(last, *wide), end=(0, *halves(last - 1)))
    finish(0, *halves(last))
    fetch_o(WBUFS - 1)

    pl.semaphore_signal(free_sem, inc=1, device_id=device(partner), device_id_type=MESH)
    for rel in others:
        for part in range(parts):
            o_arrival(rel, part).wait_recv()
    pl.semaphore_wait(free_sem, 1)

    for kind in range(2):
        for a in range(CHIPS):
            to_partner(kind, a, 1 - core).wait_recv()
        for h in range(8):
            acc[pl.ds(kind * 8 * rows + h, rows, stride=8), :] = kturn[kind, h, :rows].astype(F32)
        flat = acc[pl.ds(kind * 8 * rows, 8 * rows), :].astype(BF16)
        (kraw, vraw)[kind][0, :rows] = flat.reshape(rows, 8, HEAD_DIM)
    new_out = (pltpu.make_async_copy(kraw.at[0, :rows], k_out, turnsem.at[0, 0]),
               pltpu.make_async_copy(vraw.at[0, :rows], v_out, turnsem.at[0, 1]))
    for c in new_out:
        c.start()

    sent, got, own = 0, out_tiles * rows, 2 * out_tiles * rows

    def lines(first, m):
        return pl.ds(pl.multiple_of(first + m * rows, rows), rows)

    def p_copy(m):
        return remote(scores.at[lines(sent, m), :], scores.at[lines(got, m), :], psend.at[m], precv.at[m], partner)

    def out_copy(m):
        cols = pl.ds(pl.multiple_of(m * TILE, TILE), TILE)
        return pltpu.make_async_copy(outst.at[rem(m, 2)], out.at[:, cols], outsem.at[m])

    def x_copy(m):
        cols = pl.ds(pl.multiple_of(m * TILE, TILE), TILE)
        return pltpu.make_async_copy(x_in.at[:, cols], xres.at[rem(m, 2)], xsem.at[3 + rem(m, 2)])

    def combine(m):
        if isinstance(m, int):
            out_copy(m - 2).wait()
        else:
            @pl.when(m >= 2)
            def _():
                out_copy(m - 2).wait()
        p_copy(m).wait_recv()
        x_copy(m).wait()
        both = scores[lines(own, m), :] + scores[lines(got, m), :]
        outst[rem(m, 2)] = (xres[rem(m, 2)].astype(F32) + both).astype(BF16)
        out_copy(m).start()

    def output(m, carry):
        @pl.when(m >= 1)
        def _():
            p_copy(m - 1).start()

        @pl.when(m >= 2)
        def _():
            combine(m - 2)

        x_copy(m).start()
        wait_tile(p1_tiles + m)
        both = multiply(p1_tiles + m)
        scores[lines(own, m), :] = jnp.where(core == 0, both[:rows], both[rows:])
        scores[lines(sent, m), :] = jnp.where(core == 0, both[rows:], both[:rows])

        @pl.when(m + WBUFS < out_tiles)
        def _():
            fetch_o(m + WBUFS)

        return carry

    lax.fori_loop(0, out_tiles, output, 0)
    p_copy(out_tiles - 1).start()
    combine(out_tiles - 2)
    combine(out_tiles - 1)

    def drain(m, carry):
        p_copy(m).wait_send()
        return carry

    lax.fori_loop(0, out_tiles, drain, 0)
    out_copy(out_tiles - 2).wait()
    out_copy(out_tiles - 1).wait()
    x_remote.wait_send()
    for p in range(1, 8):
        for kind in range(2):
            kv_copy(p, kind).wait_send()
    for rel in others:
        new_copy(rel, 1).wait_send()
        for part in range(parts):
            o_copy(rel, part).wait_send()
    for a in range(CHIPS):
        to_partner(1, a, core).wait_send()
    for c in new_out:
        c.wait()


def block(x, k_cache, v_cache, ln_gain, k_gain, q_gain, cos_tab, sin_tab, w_q, w_k, w_v, w_o):
    rows, hid = x.shape
    seg = k_cache.shape[0]
    width = w_q.shape[1] // 8
    pair, new = 2 * rows, 8 * rows
    parts = width // TILE
    tiles = 8 * parts
    out_tiles = hid // TILE
    keys_b = 2 * seg + new
    cached = 8 * seg
    flops = 4 * (cached + new) * 8 * rows * width + 8 * rows * hid * width * 2
    hbm = pl.BlockSpec(memory_space=pl.ANY)
    vmem = pl.BlockSpec(memory_space=pltpu.VMEM)
    dma = pltpu.SemaphoreType.DMA
    return pl.pallas_call(
        functools.partial(block_kernel, rows, seg, width),
        out_shape=(
            jax.ShapeDtypeStruct((rows, hid), BF16),
            jax.ShapeDtypeStruct((rows, 8, HEAD_DIM), BF16),
            jax.ShapeDtypeStruct((rows, 8, HEAD_DIM), BF16),
            jax.ShapeDtypeStruct((8, seg, HEAD_DIM), BF16),
            jax.ShapeDtypeStruct((8, HEAD_DIM, seg), BF16),
        ),
        in_specs=[hbm, hbm, hbm, vmem, vmem, vmem, vmem, vmem, hbm, hbm, hbm, hbm],
        out_specs=(hbm,) * 5,
        scratch_shapes=[
            pltpu.VMEM((2, rows, TILE), BF16),
            pltpu.VMEM((1, hid + 2 * HEAD_DIM), F32),
            pltpu.VMEM((pair, hid), BF16),
            pltpu.VMEM((WBUFS, hid, TILE), BF16),
            pltpu.VMEM((pair, TILE), BF16),
            pltpu.VMEM((5, pair, width), BF16),
            pltpu.VMEM((4, HEAD_DIM, pair), BF16),
            pltpu.VMEM((4, pair, width), BF16),
            pltpu.VMEM((cached + new, HEAD_DIM), BF16),
            pltpu.VMEM((HEAD_DIM, cached + new), BF16),
            pltpu.VMEM((max(keys_b, 3 * out_tiles * rows), TILE), F32),
            pltpu.VMEM((tiles * HEADS * HEAD_DIM, rows), F32),
            pltpu.VMEM((RAWS, seg // 8, 8, HEAD_DIM), BF16),
            pltpu.VMEM((RAWS, seg // 8, 8, HEAD_DIM), BF16),
            pltpu.VMEM((2, 8, seg // 8, HEAD_DIM), BF16),
            pltpu.VMEM((2, 8, HEAD_DIM, seg // 8), BF16),
            pltpu.VMEM((tiles, 1, TILE), F32),
            pltpu.VMEM((tiles, 1, TILE), F32),
            pltpu.VMEM((1, TILE), F32),
            pltpu.VMEM((8, TILE), F32),
            pltpu.VMEM((SUB, rows), jnp.int32),
            pltpu.VMEM((2, rows, TILE), BF16),
            dma((WBUFS, 4)),
            dma((5,)),
            dma((4, parts)), dma((4, parts)),
            dma((2, 8)), dma((2, 8)),
            dma((2, 4)), dma((2, 4)),
            dma((4, parts)), dma((4, parts)),
            dma((2, 4)), dma((2, 4)),
            dma((out_tiles,)), dma((out_tiles,)),
            dma((out_tiles,)),
            dma((4, RAWS)),
            pltpu.SemaphoreType.REGULAR,
        ],
        compiler_params=pltpu.CompilerParams(
            collective_id=0, has_side_effects=True, vmem_limit_bytes=67043328),
        cost_estimate=pl.CostEstimate(flops=flops, bytes_accessed=200 * 1024 * 1024, transcendentals=flops // 512),
        name="block",
    )(x, k_cache, v_cache, ln_gain, k_gain, q_gain, cos_tab, sin_tab, w_q, w_k, w_v, w_o)


def hand_over(*results):
    pieces = 4

    def copy(*refs):
        count = len(results)
        sources, targets, held, sems = refs[:count], refs[count:2 * count], refs[2 * count:3 * count], refs[-1]
        copies = []
        for i, (source, target, middle) in enumerate(zip(sources, targets, held)):
            some = source.shape[0] // pieces
            for j in range(pieces):
                at = pl.ds(j * some, some)
                copies.append((pltpu.make_async_copy(source.at[at], middle.at[at], sems.at[0, i, j]),
                               pltpu.make_async_copy(middle.at[at], target.at[at], sems.at[1, i, j])))
        for into, _ in copies:
            into.start()
        for into, back in copies:
            into.wait()
            back.start()
        for _, back in copies:
            back.wait()

    hbm = pl.BlockSpec(memory_space=pl.ANY)
    return pl.pallas_call(
        copy,
        out_shape=tuple(jax.ShapeDtypeStruct(a.shape, a.dtype) for a in results),
        in_specs=[hbm] * len(results),
        out_specs=(hbm,) * len(results),
        scratch_shapes=[*(pltpu.VMEM(a.shape, a.dtype) for a in results),
                        pltpu.SemaphoreType.DMA((2, len(results), pieces))],
        name="hand_over",
    )(*results)


def solution(mesh):
    cp_size = mesh.shape['cp']
    row_spec = P(('dp', 'cp'), None)
    cache_spec = P(('dp', 'cp'), None, None)
    whole = P()

    def device_step(x_rows, k_cache, v_cache, ln_gain, w_q, w_k, w_v, w_o, q_gain, k_gain):
        rows = x_rows.shape[0]
        prefix_len = k_cache.shape[0] * cp_size
        chip = lax.axis_index('cp') // 2
        positions = (prefix_len + chip * 2 * rows + jnp.arange(2 * rows)).astype(F32)
        lane = jnp.arange(HEAD_DIM)
        half = HEAD_DIM // 2
        inv_freq = ROPE_THETA ** (-(lane % half).astype(F32) * (2.0 / HEAD_DIM))
        angles = positions[:, None] * inv_freq[None, :]
        cos_tab = jnp.cos(angles)
        sin_tab = jnp.sin(angles) * jnp.where(lane < half, -1.0, 1.0)[None, :]
        out, k_new, v_new, _, _ = block(
            x_rows, k_cache, v_cache, ln_gain.reshape(-1, HEAD_DIM), k_gain[None, :], q_gain[None, :], cos_tab, sin_tab, w_q, w_k, w_v, w_o)
        return hand_over(out, k_new, v_new)

    return jax.shard_map(device_step, mesh=mesh, in_specs=(row_spec, cache_spec, cache_spec, whole, whole, whole, whole, whole, whole, whole), out_specs=(row_spec, cache_spec, cache_spec), check_vma=False)
```

```python
import functools
import math

import jax
import jax.numpy as jnp
from jax import lax
from jax.experimental import pallas as pl
from jax.experimental.pallas import tpu as pltpu
from jax.sharding import PartitionSpec as P

HEAD_DIM = 128
ROPE_THETA = 1.0e6
NORM_EPS = 1.0e-6
MESH = pl.DeviceIdType.MESH
F32 = jnp.float32
BF16 = jnp.bfloat16

ORD = (0, 1, 2, 4, 3, 5, 6, 7)
SUB = 256
TILE = 512
HEADS = TILE // HEAD_DIM
WBUFS = 3
RAWS = 3
CHIPS = 4


def div(a, b):
    return a // b if isinstance(a, int) else lax.div(a, jnp.int32(b))


def rem(a, b):
    return a % b if isinstance(a, int) else lax.rem(a, jnp.int32(b))


def flip(me, rel):
    out = 0
    for bit in (1, 2, 4):
        mine = rem(div(me, bit), 2)
        out = out + bit * ((1 - mine) if rel & bit else mine)
    return out


def flip_chip(chip, rel):
    return rem(rem(chip, 2) + rem(rel, 2), 2) + 2 * rem(div(chip, 2) + div(rel, 2), 2)


def block_kernel(rows, seg, width,
                 x_in, k_in, v_in, ln_in, kg_in, qg_in, cos_in, sin_in, wq_in, wk_in, wv_in, wo_in,
                 out, k_out, v_out, kt, vt,
                 xres, gains, hbuf, wbuf, raw, stage, vstage, qbuf, kbuf, vbuf, scores, acc, kraw, vraw, kturn, vturn, peak_ref, sum_ref, fade_ref, chunk_max, ahead_ref, outst,
                 wsem, xsem, qsend, qrecv, kvsend, kvrecv, nsend, nrecv, osend, orecv, ksend, krecv, psend, precv, outsem, turnsem,
                 free_sem):
    dp = lax.axis_index("dp")
    me = lax.axis_index("cp")
    chip, core = div(me, 2), rem(me, 2)
    hid = wbuf.shape[1]
    pair = 2 * rows
    new = 8 * rows
    parts = width // TILE
    per_chip = 2 * parts
    tiles = 4 * per_chip
    keys_a = 2 * seg
    keys_b = 2 * seg + new
    coef = math.log2(math.e) * HEAD_DIM ** -0.5
    neg = float("-inf")
    q_tiles = 4 * parts
    p1_tiles = q_tiles + 2
    out_tiles = hid // TILE
    cached = 8 * seg
    others = range(1, CHIPS)
    chunk = hid // 4
    turns = 8
    cleared = acc.shape[0] // (p1_tiles - turns)
    depth = seg // turns

    def device(index):
        return (dp, index)

    partner = flip(me, 1)

    my_rows = pl.ds(pl.multiple_of(core * rows, rows), rows)
    other_rows = pl.ds(pl.multiple_of((1 - core) * rows, rows), rows)
    x_local = pltpu.make_async_copy(x_in, hbuf.at[my_rows, :], xsem.at[0])
    x_local.start()

    barrier = pltpu.get_barrier_semaphore()
    for rel in range(1, 8):
        pl.semaphore_signal(barrier, inc=1, device_id=device(flip(me, rel)), device_id_type=MESH)

    def remote(src, dst, send, recv, index):
        return pltpu.make_async_remote_copy(
            src_ref=src, dst_ref=dst, send_sem=send, recv_sem=recv, device_id=device(index), device_id_type=MESH)

    def tile_of(ref, slot, a):
        return ref.at[slot, pl.ds(a * chunk, chunk), :]

    def fetch_kv(ref, n):
        slot = rem(n, WBUFS)
        for a in range(CHIPS):
            first = pl.multiple_of((2 * a + core) * HEAD_DIM, HEAD_DIM)
            pltpu.make_async_copy(ref.at[:, pl.ds(first, HEAD_DIM)],
                                  wbuf.at[slot, :, pl.ds(a * HEAD_DIM, HEAD_DIM)], wsem.at[slot, a]).start()

    def fetch_q(n):
        slot = rem(n, WBUFS)
        g, part = div(n - 1, parts), rem(n - 1, parts)
        head = 2 * flip_chip(chip, rem(g + 1, 4)) + core
        first = pl.multiple_of(head * width + part * TILE, TILE)
        for a in range(CHIPS):
            pltpu.make_async_copy(wq_in.at[pl.ds(a * chunk, chunk), pl.ds(first, TILE)],
                                  tile_of(wbuf, slot, a), wsem.at[slot, a]).start()

    def fetch_o(m):
        slot = rem(p1_tiles + m, WBUFS)
        first = pl.multiple_of(m * TILE, TILE)
        for a in range(CHIPS):
            top = pl.multiple_of((2 * a + core) * width, width)
            pltpu.make_async_copy(wo_in.at[pl.ds(top, width), pl.ds(first, TILE)],
                                  tile_of(wbuf, slot, a), wsem.at[slot, a]).start()

    def wait_tile(n):
        slot = rem(n, WBUFS)
        for a in range(CHIPS):
            pltpu.make_async_copy(tile_of(wbuf, slot, a), tile_of(wbuf, slot, a), wsem.at[slot, a]).wait()

    def turn_in(c):
        where = pl.ds(pl.multiple_of(c * depth, depth), depth)
        slot = rem(c, RAWS)
        return (pltpu.make_async_copy(k_in.at[where], kraw.at[slot], turnsem.at[0, slot]),
                pltpu.make_async_copy(v_in.at[where], vraw.at[slot], turnsem.at[1, slot]))

    def turn_out(c):
        where = pl.ds(pl.multiple_of(c * depth, depth), depth)
        slot = rem(c, 2)
        return (pltpu.make_async_copy(kturn.at[slot], kt.at[:, where, :], turnsem.at[2, slot]),
                pltpu.make_async_copy(vturn.at[slot], vt.at[:, :, where], turnsem.at[3, slot]))

    def turn(c):
        slot, here = rem(c, 2), rem(c, RAWS)
        acc[pl.ds(0, 8 * depth), :] = kraw[here].astype(F32).reshape(8 * depth, HEAD_DIM)
        acc[pl.ds(8 * depth, 8 * depth), :] = vraw[here].astype(F32).reshape(8 * depth, HEAD_DIM)
        for h in range(8):
            kturn[slot, h] = acc[pl.ds(h, depth, stride=8), :].astype(BF16)
            vturn[slot, h] = acc[pl.ds(8 * depth + h, depth, stride=8), :].T.astype(BF16)

    x_remote = remote(x_in, hbuf.at[my_rows, :], xsem.at[1], xsem.at[2], partner)
    x_local.wait()
    for c in turn_in(0):
        c.start()
    fetch_kv(wk_in, 0)
    for piece in range(1, RAWS):
        for c in turn_in(piece):
            c.start()
    pl.semaphore_wait(barrier, 7)
    x_remote.start()
    fetch_q(1)
    fetch_q(2)

    def kv_copy(p, kind):
        peer = flip(me, ORD[p])
        if kind == 0:
            src, dst = kt.at[peer], kbuf.at[pl.ds(p * seg, seg), :]
        else:
            src, dst = vt.at[peer], vbuf.at[:, pl.ds(p * seg, seg)]
        if p == 0:
            return pltpu.make_async_copy(src, dst, kvrecv.at[kind, 0])
        return remote(src, dst, kvsend.at[kind, p], kvrecv.at[kind, p], peer)

    def kv_send(pair_index):
        for p in (2 * pair_index, 2 * pair_index + 1):
            for kind in range(2):
                kv_copy(p, kind).start()

    def kv_wait(p):
        for kind in range(2):
            if p == 0:
                kv_copy(p, kind).wait()
            else:
                kv_copy(p, kind).wait_recv()

    def normalise(first_row):
        def some(i, carry):
            at = pl.multiple_of(first_row + i * 32, 32)
            wide = hbuf[pl.ds(at, 32), :].astype(F32)
            mean_sq = jnp.sum(wide * wide, axis=-1, keepdims=True) * (1.0 / hid)
            hbuf[pl.ds(at, 32), :] = (wide * lax.rsqrt(mean_sq + NORM_EPS) * gains[:, :hid]).astype(BF16)
            return carry
        lax.fori_loop(0, rows // 32, some, 0)

    for r in range(hid // HEAD_DIM):
        gains[:, r * HEAD_DIM:(r + 1) * HEAD_DIM] = ln_in[r:r + 1, :].astype(F32)
    gains[:, hid:hid + HEAD_DIM] = kg_in[...].astype(F32)
    gains[:, hid + HEAD_DIM:] = qg_in[...].astype(F32)
    normalise(core * rows)
    for c in turn_in(0):
        c.wait()
    turn(0)
    for c in (*turn_out(0), *turn_in(RAWS)):
        c.start()
    x_remote.wait_recv()
    normalise((1 - core) * rows)

    def multiply(n):
        slot = rem(n, WBUFS)
        return jnp.dot(hbuf[...], wbuf[slot], preferred_element_type=F32)

    def rotate(e):
        group, part = div(e + parts - 1, parts), rem(e + parts - 1, parts)
        gain = gains[:, pl.ds(pl.multiple_of(hid + jnp.minimum(e, 1) * HEAD_DIM, HEAD_DIM), HEAD_DIM)]
        cos_tab, sin_tab = cos_in[...], sin_in[...]
        done = []
        for h in range(HEADS):
            vals = raw[:, h * HEAD_DIM:(h + 1) * HEAD_DIM].astype(F32)
            mean_sq = jnp.sum(vals * vals, axis=-1, keepdims=True) * (1.0 / HEAD_DIM)
            vals = vals * lax.rsqrt(mean_sq + NORM_EPS) * gain
            done.append((vals * cos_tab + pltpu.roll(vals, HEAD_DIM // 2, 1) * sin_tab).astype(BF16))
        done = jnp.concatenate(done, axis=1)
        where = pl.ds(pl.multiple_of(part * TILE, TILE), TILE)
        stage[group, :, where] = done
        qbuf[0, :, where] = done

    def q_copy(rel, part):
        cols = pl.ds(pl.multiple_of(part * TILE, TILE), TILE)
        return remote(stage.at[rel, :, cols], qbuf.at[rel, :, cols], qsend.at[rel, part], qrecv.at[rel, part],
                      2 * flip_chip(chip, rel) + core)

    def new_copy(rel, kind):
        other = flip_chip(chip, rel)
        here = pl.ds(pl.multiple_of(cached + chip * pair, pair), pair)
        if kind == 0:
            first = pl.multiple_of((parts - 1) * TILE + other * HEAD_DIM, HEAD_DIM)
            src, dst = stage.at[0, :, pl.ds(first, HEAD_DIM)], kbuf.at[here, :]
        else:
            src, dst = vstage.at[other], vbuf.at[:, here]
        return remote(src, dst, nsend.at[kind, rel], nrecv.at[kind, rel], 2 * other + core)

    def new_heads(kind, a):
        if kind == 0:
            return stage.at[0, :, pl.ds((parts - 1) * TILE + a * HEAD_DIM, HEAD_DIM)]
        return raw.at[:, pl.ds(a * HEAD_DIM, HEAD_DIM)]

    def to_partner(kind, a, parity):
        dst = kturn.at[kind, 2 * a + parity, pl.ds(0, rows), :]
        return remote(new_heads(kind, a).at[other_rows, :], dst, ksend.at[kind, a], krecv.at[kind, a], partner)

    wait_tile(0)
    raw[...] = multiply(0).astype(BF16)
    fetch_q(3)

    def project(turning, n, carry):
        @pl.when(n == 2)
        def _():
            for rel in others:
                new_copy(rel, 0).start()

        @pl.when((n >= 3) & (n < 3 + 3 * parts))
        def _():
            e = n - 2
            q_copy(div(e + parts - 1, parts), rem(e + parts - 1, parts)).start()

        if turning:
            for c in turn_in(n):
                c.wait()

            @pl.when(n >= 2)
            def _():
                for c in turn_out(n - 2):
                    c.wait()
        else:
            @pl.when(n == turns)
            def _():
                for c in (*turn_out(turns - 2), *turn_out(turns - 1)):
                    c.wait()
                for p in range(2):
                    for kind in range(2):
                        kv_copy(p, kind).start()

            @pl.when(n == 3 + 3 * parts)
            def _():
                kv_send(1)

        wait_tile(n)
        rotate(n - 1)
        if turning:
            turn(n)
        else:
            acc[pl.ds(pl.multiple_of((n - turns) * cleared, cleared), cleared), :] = jnp.zeros((cleared, rows), F32)
        raw[...] = multiply(n).astype(BF16)
        if turning:
            for c in turn_out(n):
                c.start()

            @pl.when(n + RAWS < turns)
            def _():
                for c in turn_in(n + RAWS):
                    c.start()

        @pl.when(n + WBUFS <= q_tiles)
        def _():
            fetch_q(n + WBUFS)

        @pl.when(n + WBUFS == q_tiles + 1)
        def _():
            fetch_kv(wv_in, q_tiles + 1)

        @pl.when((n + WBUFS >= p1_tiles) & (n + WBUFS < p1_tiles + WBUFS - 1))
        def _():
            fetch_o(n + WBUFS - p1_tiles)

        return carry

    lax.fori_loop(1, turns, functools.partial(project, True), 0)
    lax.fori_loop(turns, p1_tiles, functools.partial(project, False), 0)

    here = pl.ds(pl.multiple_of(cached + chip * pair, pair), pair)
    for a in range(CHIPS):
        vstage[a] = raw[:, a * HEAD_DIM:(a + 1) * HEAD_DIM].astype(F32).T.astype(BF16)
    kbuf[here, :] = stage[0, :, pl.ds(pl.multiple_of((parts - 1) * TILE + chip * HEAD_DIM, HEAD_DIM), HEAD_DIM)]
    vbuf[:, here] = vstage[chip]

    def acc_rows(t, h):
        return pl.ds(pl.multiple_of((t * HEADS + h) * HEAD_DIM, HEAD_DIM), HEAD_DIM)

    def init(t, carry):
        peak_ref[t] = jnp.full((1, TILE), neg, F32)
        sum_ref[t] = jnp.zeros((1, TILE), F32)
        return carry

    lax.fori_loop(0, tiles, init, 0)
    ahead_ref[...] = (lax.broadcasted_iota(jnp.int32, (SUB, rows), 0)
                      - lax.broadcasted_iota(jnp.int32, (SUB, rows), 1))
    for rel in others:
        new_copy(rel, 1).start()

    def q_tile(rel, half, part):
        some_rows = pl.ds(pl.multiple_of(half * rows, rows), rows)
        block = qbuf[rel, some_rows, pl.ds(pl.multiple_of(part * TILE, TILE), TILE)]
        return jnp.concatenate([block[:, h * HEAD_DIM:(h + 1) * HEAD_DIM] for h in range(HEADS)], axis=0)

    probs = wbuf.at[(p1_tiles + WBUFS - 1) % WBUFS]

    def step(pv=None, sm=None, qk=None, end=None):
        if end is not None:
            finish(*end)
        if pv is not None:
            t_pv, base_pv, keys_pv = pv
            fade_pv = fade_ref[...]
        if sm is not None:
            t_sm, keys_sm = sm
            old = peak_ref[t_sm]
            top = jnp.maximum(old, jnp.max(chunk_max[...], axis=0, keepdims=True) * coef)
            fade = jnp.exp2(old - top)
            peak_ref[t_sm] = top
        if qk is not None:
            rel_qk, half_qk, part_qk, base_qk, keys_qk, has_new = qk
            q = q_tile(rel_qk, half_qk, part_qk)
            first_row = flip_chip(chip, rel_qk) * pair + half_qk * rows if has_new else None

        def scores_of(s):
            k_part = kbuf[pl.ds(pl.multiple_of(base_qk + s * SUB, SUB), SUB), :]
            return lax.dot_general(k_part, q, (((1,), (1,)), ((), ())), preferred_element_type=F32)

        total = None
        values = None
        peaks = None
        most = max(pv[2] if pv else 0, sm[1] if sm else 0, qk[4] if qk else 0)
        for s in range(most // SUB):
            lines = slice(s * SUB, (s + 1) * SUB)
            if qk is not None and s * SUB < keys_qk and has_new:
                sc = scores_of(s)
            if pv is not None and s * SUB < keys_pv:
                v_part = vbuf[:, pl.ds(pl.multiple_of(base_pv + s * SUB, SUB), SUB)]
                o_part = jnp.dot(v_part, probs[lines, :], preferred_element_type=F32)
                values = o_part if values is None else values + o_part
            if sm is not None and s * SUB < keys_sm:
                w = jnp.exp2(scores[lines, :] * coef - top)
                part = jnp.sum(w.reshape(SUB // 8, 8, TILE), axis=0)
                total = part if total is None else total + part
                probs[lines, :] = w.astype(BF16)
            if qk is not None and s * SUB < keys_qk:
                if not has_new:
                    sc = scores_of(s)
                if has_new and s * SUB >= keys_a:
                    seen = ahead_ref[...] <= first_row - (s * SUB - keys_a)
                    sc = jnp.concatenate(
                        [jnp.where(seen, sc[:, h * rows:(h + 1) * rows], neg) for h in range(HEADS)], axis=1)
                scores[lines, :] = sc
                part = jnp.max(sc.reshape(SUB // 8, 8, TILE), axis=0)
                peaks = part if peaks is None else jnp.maximum(peaks, part)
        if qk is not None:
            chunk_max[...] = peaks
        if sm is not None:
            sum_ref[t_sm] = sum_ref[t_sm] * fade + jnp.sum(total, axis=0, keepdims=True)
            fade_ref[...] = fade
        if pv is not None:
            for h in range(HEADS):
                cols = slice(h * rows, (h + 1) * rows)
                acc[acc_rows(t_pv, h), :] = acc[acc_rows(t_pv, h), :] * fade_pv[:, cols] + values[:, cols]

    def finish(rel, half, part):
        t = rel * per_chip + 2 * part + half
        some_rows = pl.ds(pl.multiple_of(half * rows, rows), rows)
        sums = sum_ref[t]
        done = jnp.concatenate(
            [(acc[acc_rows(t, h), :] / sums[:, h * rows:(h + 1) * rows]).T.astype(BF16) for h in range(HEADS)], axis=1)
        stage[rel, some_rows, pl.ds(pl.multiple_of(part * TILE, TILE), TILE)] = done
        hbuf[some_rows, pl.ds(pl.multiple_of(chip * width + part * TILE, TILE), TILE)] = done

    kv_wait(0)
    kv_wait(1)
    for kind in range(2):
        for a in range(CHIPS):
            kturn[kind, 2 * a + core, :rows] = new_heads(kind, a)[my_rows, :]
            to_partner(kind, a, core).start()

    def halves(u):
        part = div(u, 2)
        return u - 2 * part, part

    step(qk=(0, 0, 0, 0, keys_a, False))
    step(sm=(0, keys_a), qk=(0, *halves(1), 0, keys_a, False))

    def below(u, limit):
        return jnp.minimum(jnp.maximum(limit - u, 0), 1)

    def group_a(g, carry):
        visit = div(g, CHIPS)
        rel = g - CHIPS * visit
        for r in others:
            @pl.when(g == r)
            def _():
                for part in range(parts):
                    q_copy(r, part).wait_recv()

        for v in (1, 2):
            @pl.when(g == CHIPS * v)
            def _():
                kv_wait(2 * v)
                kv_wait(2 * v + 1)

        @pl.when(g == 3)
        def _():
            kv_send(2)

        @pl.when(g == 6)
        def _():
            kv_send(3)

        def body_a(u, carry):
            t = rel * per_chip + u
            wrap = below(t, 2)
            step(pv=(t - 2 + tiles * wrap, (visit - wrap) * keys_a, keys_a),
                 sm=(t - 1 + tiles * below(t, 1), keys_a),
                 qk=(rel, *halves(u), visit * keys_a, keys_a, False))
            return carry

        lax.fori_loop(2 * below(g, 1), per_chip, body_a, carry)
        return carry

    lax.fori_loop(0, 3 * CHIPS, group_a, 0)

    kv_wait(6)
    kv_wait(7)
    for rel in others:
        new_copy(rel, 0).wait_recv()
        new_copy(rel, 1).wait_recv()
        new_copy(rel, 0).wait_send()
        for part in range(parts):
            q_copy(rel, part).wait_send()
    for a in range(CHIPS):
        to_partner(0, a, core).wait_send()

    def o_copy(rel, part):
        cols = pl.ds(pl.multiple_of(part * TILE, TILE), TILE)
        there = pl.ds(pl.multiple_of(chip * width + part * TILE, TILE), TILE)
        return remote(stage.at[rel, :, cols], hbuf.at[:, there], osend.at[rel, part], orecv.at[rel, part],
                      2 * flip_chip(chip, rel) + core)

    def o_arrival(rel, part):
        there = pl.ds(pl.multiple_of(flip_chip(chip, rel) * width + part * TILE, TILE), TILE)
        return remote(hbuf.at[:, there], hbuf.at[:, there], osend.at[rel, part], orecv.at[rel, part],
                      2 * flip_chip(chip, rel) + core)

    base_b = 3 * keys_a
    wide = (base_b, keys_b)

    step(pv=(tiles - 2, 2 * keys_a, keys_a), sm=(tiles - 1, keys_a), qk=(3, 0, 0, *wide, True))
    step(pv=(tiles - 1, 2 * keys_a, keys_a), sm=(3 * per_chip, keys_b), qk=(3, *halves(1), *wide, True))
    step(pv=(3 * per_chip, *wide), sm=(3 * per_chip + 1, keys_b), qk=(3, *halves(2), *wide, True))

    def group_b(g, carry):
        rel = 3 - g

        def body_b(u, carry):
            n = g * per_chip + u

            @pl.when((rem(n, 2) == 1) & (n >= 5) & (n < 5 + 3 * per_chip))
            def _():
                done = n - 5
                o_copy(3 - div(done, per_chip), div(rem(done, per_chip), 2)).start()

            t = rel * per_chip + u
            early = below(u, 3)
            step(pv=(t - 2 + 2 * per_chip * below(u, 2), *wide),
                 sm=(t - 1 + 2 * per_chip * below(u, 1), keys_b),
                 qk=(rel, *halves(u), *wide, True),
                 end=(rel + early, *halves(u - 3 + per_chip * early)))
            return carry

        lax.fori_loop(3 * below(g, 1), per_chip, body_b, carry)
        return carry

    lax.fori_loop(0, CHIPS, group_b, 0)
    last = per_chip - 1
    step(pv=(last - 1, *wide), sm=(last, keys_b), end=(0, *halves(last - 2)))
    step(pv=(last, *wide), end=(0, *halves(last - 1)))
    finish(0, *halves(last))
    fetch_o(WBUFS - 1)

    pl.semaphore_signal(free_sem, inc=1, device_id=device(partner), device_id_type=MESH)
    for rel in others:
        for part in range(parts):
            o_arrival(rel, part).wait_recv()
    pl.semaphore_wait(free_sem, 1)

    for kind in range(2):
        for a in range(CHIPS):
            to_partner(kind, a, 1 - core).wait_recv()
        for h in range(8):
            acc[pl.ds(kind * 8 * rows + h, rows, stride=8), :] = kturn[kind, h, :rows].astype(F32)
        flat = acc[pl.ds(kind * 8 * rows, 8 * rows), :].astype(BF16)
        (kraw, vraw)[kind][0, :rows] = flat.reshape(rows, 8, HEAD_DIM)
    new_out = (pltpu.make_async_copy(kraw.at[0, :rows], k_out, turnsem.at[0, 0]),
               pltpu.make_async_copy(vraw.at[0, :rows], v_out, turnsem.at[0, 1]))
    for c in new_out:
        c.start()

    sent, got, own = 0, out_tiles * rows, 2 * out_tiles * rows

    def lines(first, m):
        return pl.ds(pl.multiple_of(first + m * rows, rows), rows)

    def p_copy(m):
        return remote(scores.at[lines(sent, m), :], scores.at[lines(got, m), :], psend.at[m], precv.at[m], partner)

    def out_copy(m):
        cols = pl.ds(pl.multiple_of(m * TILE, TILE), TILE)
        return pltpu.make_async_copy(outst.at[rem(m, 2)], out.at[:, cols], outsem.at[m])

    def x_copy(m):
        cols = pl.ds(pl.multiple_of(m * TILE, TILE), TILE)
        return pltpu.make_async_copy(x_in.at[:, cols], xres.at[rem(m, 2)], xsem.at[3 + rem(m, 2)])

    def combine(m):
        if isinstance(m, int):
            out_copy(m - 2).wait()
        else:
            @pl.when(m >= 2)
            def _():
                out_copy(m - 2).wait()
        p_copy(m).wait_recv()
        x_copy(m).wait()
        both = scores[lines(own, m), :] + scores[lines(got, m), :]
        outst[rem(m, 2)] = (xres[rem(m, 2)].astype(F32) + both).astype(BF16)
        out_copy(m).start()

    def output(m, carry):
        @pl.when(m >= 1)
        def _():
            p_copy(m - 1).start()

        @pl.when(m >= 2)
        def _():
            combine(m - 2)

        x_copy(m).start()
        wait_tile(p1_tiles + m)
        both = multiply(p1_tiles + m)
        scores[lines(own, m), :] = jnp.where(core == 0, both[:rows], both[rows:])
        scores[lines(sent, m), :] = jnp.where(core == 0, both[rows:], both[:rows])

        @pl.when(m + WBUFS < out_tiles)
        def _():
            fetch_o(m + WBUFS)

        return carry

    lax.fori_loop(0, out_tiles, output, 0)
    p_copy(out_tiles - 1).start()
    combine(out_tiles - 2)
    combine(out_tiles - 1)

    def drain(m, carry):
        p_copy(m).wait_send()
        return carry

    lax.fori_loop(0, out_tiles, drain, 0)
    out_copy(out_tiles - 2).wait()
    out_copy(out_tiles - 1).wait()
    x_remote.wait_send()
    for p in range(1, 8):
        for kind in range(2):
            kv_copy(p, kind).wait_send()
    for rel in others:
        new_copy(rel, 1).wait_send()
        for part in range(parts):
            o_copy(rel, part).wait_send()
    for a in range(CHIPS):
        to_partner(1, a, core).wait_send()
    for c in new_out:
        c.wait()


def block(x, k_cache, v_cache, ln_gain, k_gain, q_gain, cos_tab, sin_tab, w_q, w_k, w_v, w_o):
    rows, hid = x.shape
    seg = k_cache.shape[0]
    width = w_q.shape[1] // 8
    pair, new = 2 * rows, 8 * rows
    parts = width // TILE
    tiles = 8 * parts
    out_tiles = hid // TILE
    keys_b = 2 * seg + new
    cached = 8 * seg
    flops = 4 * (cached + new) * 8 * rows * width + 8 * rows * hid * width * 2
    hbm = pl.BlockSpec(memory_space=pl.ANY)
    vmem = pl.BlockSpec(memory_space=pltpu.VMEM)
    dma = pltpu.SemaphoreType.DMA
    return pl.pallas_call(
        functools.partial(block_kernel, rows, seg, width),
        out_shape=(
            jax.ShapeDtypeStruct((rows, hid), BF16),
            jax.ShapeDtypeStruct((rows, 8, HEAD_DIM), BF16),
            jax.ShapeDtypeStruct((rows, 8, HEAD_DIM), BF16),
            jax.ShapeDtypeStruct((8, seg, HEAD_DIM), BF16),
            jax.ShapeDtypeStruct((8, HEAD_DIM, seg), BF16),
        ),
        in_specs=[hbm, hbm, hbm, vmem, vmem, vmem, vmem, vmem, hbm, hbm, hbm, hbm],
        out_specs=(hbm,) * 5,
        scratch_shapes=[
            pltpu.VMEM((2, rows, TILE), BF16),
            pltpu.VMEM((1, hid + 2 * HEAD_DIM), F32),
            pltpu.VMEM((pair, hid), BF16),
            pltpu.VMEM((WBUFS, hid, TILE), BF16),
            pltpu.VMEM((pair, TILE), BF16),
            pltpu.VMEM((5, pair, width), BF16),
            pltpu.VMEM((4, HEAD_DIM, pair), BF16),
            pltpu.VMEM((4, pair, width), BF16),
            pltpu.VMEM((cached + new, HEAD_DIM), BF16),
            pltpu.VMEM((HEAD_DIM, cached + new), BF16),
            pltpu.VMEM((max(keys_b, 3 * out_tiles * rows), TILE), F32),
            pltpu.VMEM((tiles * HEADS * HEAD_DIM, rows), F32),
            pltpu.VMEM((RAWS, seg // 8, 8, HEAD_DIM), BF16),
            pltpu.VMEM((RAWS, seg // 8, 8, HEAD_DIM), BF16),
            pltpu.VMEM((2, 8, seg // 8, HEAD_DIM), BF16),
            pltpu.VMEM((2, 8, HEAD_DIM, seg // 8), BF16),
            pltpu.VMEM((tiles, 1, TILE), F32),
            pltpu.VMEM((tiles, 1, TILE), F32),
            pltpu.VMEM((1, TILE), F32),
            pltpu.VMEM((8, TILE), F32),
            pltpu.VMEM((SUB, rows), jnp.int32),
            pltpu.VMEM((2, rows, TILE), BF16),
            dma((WBUFS, 4)),
            dma((5,)),
            dma((4, parts)), dma((4, parts)),
            dma((2, 8)), dma((2, 8)),
            dma((2, 4)), dma((2, 4)),
            dma((4, parts)), dma((4, parts)),
            dma((2, 4)), dma((2, 4)),
            dma((out_tiles,)), dma((out_tiles,)),
            dma((out_tiles,)),
            dma((4, RAWS)),
            pltpu.SemaphoreType.REGULAR,
        ],
        compiler_params=pltpu.CompilerParams(
            collective_id=0, has_side_effects=True, vmem_limit_bytes=67043328),
        cost_estimate=pl.CostEstimate(flops=flops, bytes_accessed=200 * 1024 * 1024, transcendentals=flops // 512),
        name="block",
    )(x, k_cache, v_cache, ln_gain, k_gain, q_gain, cos_tab, sin_tab, w_q, w_k, w_v, w_o)


def hand_over(*results):
    pieces = 4

    def copy(*refs):
        count = len(results)
        sources, targets, held, sems = refs[:count], refs[count:2 * count], refs[2 * count:3 * count], refs[-1]
        copies = []
        for i, (source, target, middle) in enumerate(zip(sources, targets, held)):
            some = source.shape[0] // pieces
            for j in range(pieces):
                at = pl.ds(j * some, some)
                copies.append((pltpu.make_async_copy(source.at[at], middle.at[at], sems.at[0, i, j]),
                               pltpu.make_async_copy(middle.at[at], target.at[at], sems.at[1, i, j])))
        for into, _ in copies:
            into.start()
        for into, back in copies:
            into.wait()
            back.start()
        for _, back in copies:
            back.wait()

    hbm = pl.BlockSpec(memory_space=pl.ANY)
    return pl.pallas_call(
        copy,
        out_shape=tuple(jax.ShapeDtypeStruct(a.shape, a.dtype) for a in results),
        in_specs=[hbm] * len(results),
        out_specs=(hbm,) * len(results),
        scratch_shapes=[*(pltpu.VMEM(a.shape, a.dtype) for a in results),
                        pltpu.SemaphoreType.DMA((2, len(results), pieces))],
        name="hand_over",
    )(*results)


def solution(mesh):
    cp_size = mesh.shape['cp']
    row_spec = P(('dp', 'cp'), None)
    cache_spec = P(('dp', 'cp'), None, None)
    whole = P()

    def device_step(x_rows, k_cache, v_cache, ln_gain, w_q, w_k, w_v, w_o, q_gain, k_gain):
        rows = x_rows.shape[0]
        prefix_len = k_cache.shape[0] * cp_size
        chip = lax.axis_index('cp') // 2
        positions = (prefix_len + chip * 2 * rows + jnp.arange(2 * rows)).astype(F32)
        lane = jnp.arange(HEAD_DIM)
        half = HEAD_DIM // 2
        inv_freq = ROPE_THETA ** (-(lane % half).astype(F32) * (2.0 / HEAD_DIM))
        angles = positions[:, None] * inv_freq[None, :]
        cos_tab = jnp.cos(angles)
        sin_tab = jnp.sin(angles) * jnp.where(lane < half, -1.0, 1.0)[None, :]
        out, k_new, v_new, _, _ = block(
            x_rows, k_cache, v_cache, ln_gain.reshape(-1, HEAD_DIM), k_gain[None, :], q_gain[None, :], cos_tab, sin_tab, w_q, w_k, w_v, w_o)
        return hand_over(out, k_new, v_new)

    return jax.shard_map(device_step, mesh=mesh, in_specs=(row_spec, cache_spec, cache_spec, whole, whole, whole, whole, whole, whole, whole), out_specs=(row_spec, cache_spec, cache_spec), check_vma=False)
```
